256 devices in a mesh: fsdp: 8 (over x, core), vocab: 32 (over y, z).
Axes of the slice: x: 4, y: 4, z: 8, core: 2. Of those that a mesh axis runs over, the one named last changes fastest.
Arguments:
- hidden_states: bfloat16 [1024, 3072], P('fsdp', 'vocab'), may hold values from -512 to 512
- head: bfloat16 [3072, 65536], P('fsdp', 'vocab'), may hold values from -0.25259074 to 0.25259074
- labels: int32 [1024], P('fsdp'), may hold values from 0 to 65535
Outputs:
- token_loss: float32 [1024], P('fsdp')
- state_grad: bfloat16 [1024, 3072], P('fsdp', 'vocab')
- head_grad: float32 [3072, 65536], P('fsdp', 'vocab')
The draws below stay inside these ranges and needn't reach their ends.
All inputs are finite; a program needn't handle non-finite values.
Results may differ from the reference program's by a relative error of at most 0.0034.
Values may be sent and summed in bfloat16 or wider, within the bound.
A program may use at most 128 MiB of HBM per device.

```python
import math
import jax
import jax.numpy as jnp
from jax import lax

D = 3072
TOK_DEV = 128
VOCAB = 65536
TOKENS = 1024


def head_matrix(key):
    base = jax.random.fold_in(key, 11)
    noise_key, spread_key = jax.random.split(base)
    noise = jnp.clip(jax.random.normal(noise_key, (D, VOCAB), jnp.float32), -5.0, 5.0)
    spread = jnp.exp(jax.random.uniform(spread_key, (VOCAB,), jnp.float32, math.log(0.8), math.log(1.25)))
    ramp = jnp.exp(math.log(2.2) * jnp.arange(VOCAB, dtype=jnp.float32) / VOCAB)
    return noise * (spread * ramp)[None, :] / math.sqrt(D)


def draw_head(key, part):
    return head_matrix(key).astype(jnp.bfloat16)


def draw_hidden_states(key, part):
    base = jax.random.fold_in(key, 23)
    scale_key, value_key = jax.random.split(base, 2)
    scale = jnp.exp(jax.random.uniform(scale_key, (TOKENS, 1), jnp.float32, math.log(0.35), math.log(1.0)))
    values = jnp.clip(jax.random.normal(value_key, (TOKENS, D), jnp.float32), -5.0, 5.0) * scale
    return values.astype(jnp.bfloat16)


def set_ends(array, rng, least, high):
    place = [jax.random.randint(jax.random.fold_in(rng, axis), (), 0, length) for axis, length in enumerate(array.shape)]
    longest = array.shape.index(max(array.shape))
    neighbour = place[:longest] + [(place[longest] + 1) % array.shape[longest]] + place[longest + 1:]
    return array.at[tuple(place)].set(least).at[tuple(neighbour)].set(high)


def setup_inputs(seed: int = 0) -> dict:
    splits = jax.random.split(jax.random.key(seed), 4)
    return {
        "hidden_states": draw_hidden_states(jax.random.fold_in(splits[3], 71), 0),
        "head": draw_head(jax.random.fold_in(splits[3], 71), 0),
        "labels": set_ends(jax.random.randint(splits[2], (TOKENS,), 0, VOCAB), jax.random.fold_in(splits[2], 1), 0, VOCAB - 1).astype(jnp.int32),
    }


def reference(hidden_states, head, labels):
    groups = TOKENS // TOK_DEV
    states = hidden_states.reshape(groups, TOK_DEV, D)
    targets = labels.reshape(groups, TOK_DEV)
    columns = jnp.arange(VOCAB, dtype=jnp.int32)

    def one_group(grad_sum, pair):
        block, wanted = pair
        logits = jnp.dot(block, head, preferred_element_type=jnp.float32)
        peak = jnp.max(logits, axis=1)
        shifted = jnp.exp(logits - peak[:, None])
        total = jnp.sum(shifted, axis=1)
        hits = wanted[:, None] == columns[None, :]
        target = jnp.sum(jnp.where(hits, logits, jnp.float32(0.0)), axis=1)
        loss = jnp.log(total) + peak - target
        errors = (shifted / total[:, None] - hits.astype(jnp.float32)).astype(jnp.bfloat16)
        state_part = lax.dot_general(errors, head, (((1,), (1,)), ((), ())), preferred_element_type=jnp.float32)
        term = lax.dot_general(block, errors, (((0,), (0,)), ((), ())), preferred_element_type=jnp.float32)
        return grad_sum + term, (loss, state_part.astype(jnp.bfloat16))

    start = jnp.zeros((D, VOCAB), jnp.float32)
    head_grad, outputs = lax.scan(one_group, start, (states, targets))
    token_loss = outputs[0].reshape(TOKENS)
    state_grad = outputs[1].reshape(TOKENS, D)
    return (token_loss, state_grad, head_grad)
```

```python
import jax
import jax.numpy as jnp
from jax import lax
from jax.sharding import PartitionSpec as P


def combine(stats):
    peaks, totals, targets = stats[:, 0], stats[:, 1], stats[:, 2]
    peak = jnp.max(peaks, axis=0)
    total = jnp.sum(totals * jnp.exp(peaks - peak[None]), axis=0)
    return jnp.stack([peak, total, jnp.sum(targets, axis=0)])


def local(hidden_states, head, labels):
    fsdp, vocab = lax.axis_size("fsdp"), lax.axis_size("vocab")
    f, v = lax.axis_index("fsdp"), lax.axis_index("vocab")
    features, width = head.shape
    tokens = hidden_states.shape[0]
    share = width // fsdp
    states = lax.all_gather(hidden_states.T, "fsdp", axis=1, tiled=True)
    states = lax.all_gather(states, "vocab", axis=0, tiled=True)
    wanted = lax.all_gather(labels, "fsdp", axis=0, tiled=True)
    weights = lax.all_to_all(head, "fsdp", split_axis=1, concat_axis=0, tiled=True)
    logits = lax.dot_general(weights, states, (((0,), (0,)), ((), ())), preferred_element_type=jnp.float32)
    rows = v * width + f * share + jnp.arange(share, dtype=jnp.int32)
    hits = rows[:, None] == wanted[None, :]
    local_target = jnp.sum(jnp.where(hits, logits, jnp.float32(0.0)), axis=0)
    local_peak = jnp.max(logits, axis=0)
    local_total = jnp.sum(jnp.exp(logits - local_peak[None, :]), axis=0)
    stats = jnp.stack([local_peak, local_total, local_target])
    stats = combine(lax.all_gather(stats, "fsdp", axis=0))
    stats = combine(lax.all_gather(stats, "vocab", axis=0))
    peak, total, target = stats[0], stats[1], stats[2]
    loss = jnp.log(total) + peak - target
    token_loss = lax.dynamic_slice_in_dim(loss, f * tokens, tokens)
    errors = (jnp.exp(logits - peak[None, :]) / total[None, :] - hits.astype(jnp.float32)).astype(jnp.bfloat16)
    errors = lax.all_gather(errors, "fsdp", axis=0, tiled=True)
    terms = jnp.dot(head, errors, preferred_element_type=jnp.float32)
    parts = vocab // fsdp
    piece = features // parts
    terms = terms.reshape(parts, piece, fsdp, tokens).transpose(2, 0, 1, 3).reshape(vocab, piece, tokens)
    summed = lax.psum_scatter(terms, "vocab", scatter_dimension=0, tiled=False).astype(jnp.bfloat16)
    moves = [
        (a * vocab + u, (u // parts) * vocab + parts * a + u % parts)
        for a in range(fsdp)
        for u in range(vocab)
    ]
    state_grad = lax.ppermute(summed, ("fsdp", "vocab"), moves).T
    mine = lax.dynamic_slice_in_dim(states, f * features, features)
    head_grad = lax.dot_general(mine, errors, (((1,), (1,)), ((), ())), preferred_element_type=jnp.float32)
    return (token_loss, state_grad, head_grad)


def solution(mesh):
    in_specs = (P("fsdp", "vocab"), P("fsdp", "vocab"), P("fsdp"))
    out_specs = (P("fsdp"), P("fsdp", "vocab"), P("fsdp", "vocab"))
    return jax.shard_map(local, mesh=mesh, in_specs=in_specs, out_specs=out_specs, check_vma=False)
```

```python
import functools

import jax
import jax.numpy as jnp
from jax import lax
from jax.experimental import pallas as pl
from jax.experimental.pallas import tpu as pltpu
from jax.sharding import PartitionSpec as P

X, Y, Z = 4, 4, 8
F32, BF16 = jnp.float32, jnp.bfloat16


def kernel(hid, head, labels, loss_out, state_out, grad_out,
           w, wl, relay, wt, h, hpad, lab, e, errs, hs, gv,
           stx, sty, stz, full, sb, ry, zs, rz, fs, fin, spad,
           load_s, w_s, wl_r, rel_r, w2_r, b1_s, b1_r, lab_s, lab_r,
           hz_s, hz_r, hy_s, hy_r, hd_s, hd_r, e_s, e_r, eh_r,
           sx_s, sx_r, sy_s, sy_r, sz_s, sz_r,
           ry_s, ry_r, rz_s, rz_r, f_s, f_r, g_s):
    f, v = lax.axis_index("fsdp"), lax.axis_index("vocab")
    x, c = lax.div(f, 2), lax.rem(f, 2)
    y, z = lax.div(v, Z), lax.rem(v, Z)
    xp, xm, xo = lax.rem(x + 1, X), lax.rem(x + 3, X), lax.rem(x + 2, X)
    yp, ym, yo = lax.rem(y + 1, Y), lax.rem(y + 3, Y), lax.rem(y + 2, Y)
    fp, fm, fo, fq = 2 * xp + c, 2 * xm + c, 2 * xo + c, 2 * x + 1 - c
    sends = []

    def at_f(g):
        return {"fsdp": g, "vocab": v}

    def at_yz(a, b):
        return {"fsdp": f, "vocab": Z * a + b}

    def send(src, dst, ssem, rsem, device):
        copy = pltpu.make_async_remote_copy(
            src_ref=src, dst_ref=dst, send_sem=ssem, recv_sem=rsem,
            device_id=device, device_id_type=pl.DeviceIdType.MESH)
        copy.start()
        sends.append(copy)

    def arrived(dst, rsem):
        pltpu.make_async_remote_copy(
            src_ref=dst, dst_ref=dst, send_sem=g_s.at[0], recv_sem=rsem,
            device_id=at_f(fq), device_id_type=pl.DeviceIdType.MESH).wait_recv()

    def home(t):
        return {"fsdp": 2 * t + lax.div(z, 4), "vocab": Z * x + 4 * c + y}

    def origin(r):
        return {"fsdp": 2 * y + lax.div(z, 4), "vocab": Z * lax.rem(z, 4) + 4 * c + r}

    own_home = jnp.logical_and(y == x, z == 4 * c + y)

    load_w = pltpu.make_async_copy(head, w, load_s.at[0])
    load_w.start()
    columns = pl.ds(pl.multiple_of(256 * f, 256), 256)
    load_own = pltpu.make_async_copy(head.at[:, columns], wl.at[f], load_s.at[1])
    load_own.start()

    barrier = pltpu.get_barrier_semaphore()

    def hello(device):
        pl.semaphore_signal(barrier, inc=1, device_id=device, device_id_type=pl.DeviceIdType.MESH)

    for k in range(1, 8):
        hello(at_f(lax.rem(f + k, 8)))
    for k in range(1, Y):
        hello(at_yz(lax.rem(y + k, Y), z))
    for k in range(1, Z):
        hello(at_yz(y, lax.rem(z + k, Z)))
    for r in range(4):
        if True:
            @pl.when(jnp.logical_not(jnp.logical_and(own_home, y == r)))
            def _():
                hello(origin(r))

    hpad[...] = jnp.zeros_like(hpad)
    hpad[:, 0:96] = hid[...].astype(F32)
    h[x, c, y, z] = hpad[...].T[0:96].astype(BF16)
    lab[f] = jnp.broadcast_to(labels[...], (8, 128))

    load_w.wait()
    pl.semaphore_wait(barrier, 7 + 3 + 7 + 4 - own_home.astype(jnp.int32))

    mine = h.at[x, c, y, z]
    for i, g in enumerate((fp, fm, fo)):
        send(mine, mine, b1_s.at[i], b1_r.at[x], at_f(g))
    for k in range(1, 8):
        send(lab.at[f], lab.at[f], lab_s.at[k], lab_r.at[f], at_f(lax.rem(f + k, 8)))

    def cols(g):
        return pl.ds(pl.multiple_of(256 * g, 256), 256)

    for d in range(2):
        send(w.at[0:192, cols(2 * xo + d)], relay.at[0, d], w_s.at[d], rel_r.at[0, d], at_f(fp))
        send(w.at[192:384, cols(2 * xo + d)], relay.at[1, d], w_s.at[2 + d], rel_r.at[1, d], at_f(fm))
    send(w.at[:, cols(fq)], wl.at[f], w_s.at[4], wl_r.at[f], at_f(fq))
    for d in range(2):
        send(w.at[:, cols(2 * xp + d)], wl.at[f], w_s.at[5 + d], wl_r.at[f], at_f(2 * xp + d))
        send(w.at[:, cols(2 * xm + d)], wl.at[f], w_s.at[7 + d], wl_r.at[f], at_f(2 * xm + d))

    def hidden_z(t):
        block = h.at[t, c, y, z]

        @pl.when(x != t)
        def _():
            arrived(block, b1_r.at[t])

        for k in range(1, Z):
            send(block, block, hz_s.at[t, k], hz_r.at[t, k], at_yz(y, lax.rem(z + k, Z)))

    for t in range(X):
        hidden_z(t)

    for d in range(2):
        arrived(relay.at[0, d], rel_r.at[0, d])
        send(relay.at[0, d], wl.at[fm, 0:192], w_s.at[9 + d], w2_r.at[0, c], at_f(2 * xp + d))
        arrived(relay.at[1, d], rel_r.at[1, d])
        send(relay.at[1, d], wl.at[fp, 192:384], w_s.at[11 + d], w2_r.at[1, c], at_f(2 * xm + d))

    def to_partner(t, row, n):
        block = h.at[t, c, row]
        send(block, block, hd_s.at[t, n], hd_r.at[t, n], at_f(fq))

    def hidden_y(t):
        for k in range(1, Z):
            arrived(h.at[t, c, y, lax.rem(z + Z - k, Z)], hz_r.at[t, k])
        block = h.at[t, c, y]
        send(block, block, hy_s.at[t, 0], hy_r.at[t, 0], at_yz(yp, z))
        send(block, block, hy_s.at[t, 1], hy_r.at[t, 1], at_yz(ym, z))
        to_partner(t, y, 0)

    def hidden_y2(t):
        arrived(h.at[t, c, ym], hy_r.at[t, 0])
        block = h.at[t, c, ym, 0:4]
        send(block, block, hy_s.at[t, 2], hy_r.at[t, 2], at_yz(yp, z))
        arrived(h.at[t, c, yp], hy_r.at[t, 1])
        block = h.at[t, c, yp, 4:8]
        send(block, block, hy_s.at[t, 3], hy_r.at[t, 3], at_yz(ym, z))
        to_partner(t, ym, 1)
        to_partner(t, yp, 2)

    def hidden_end(t):
        arrived(h.at[t, c, yo, 0:4], hy_r.at[t, 2])
        arrived(h.at[t, c, yo, 4:8], hy_r.at[t, 3])
        to_partner(t, yo, 3)

    def hidden_all(t):
        for n, row in enumerate((y, ym, yp, yo)):
            arrived(h.at[t, 1 - c, row], hd_r.at[t, n])

    hidden_y(0)
    hidden_y(1)
    hidden_y2(0)
    hidden_y(2)
    hidden_end(0)
    hidden_y2(1)

    load_own.wait()
    for g in (fq, 2 * xp, 2 * xp + 1, 2 * xm, 2 * xm + 1):
        arrived(wl.at[g], wl_r.at[g])
    for d in range(2):
        arrived(wl.at[2 * xo + d, 0:192], w2_r.at[0, d])
        arrived(wl.at[2 * xo + d, 192:384], w2_r.at[1, d])
    for g in range(8):
        wt[:, 384 * g:384 * g + 384] = wl[g].T
    for k in range(1, 8):
        g = lax.rem(f + k, 8)
        arrived(lab.at[g], lab_r.at[g])

    def wanted(t):
        return jnp.concatenate([lab[2 * t, 0:1, :], lab[2 * t + 1, 0:1, :]], axis=1)

    def rows_of(g):
        return v * 2048 + g * 256 + lax.broadcasted_iota(jnp.int32, (256, 256), 0)

    def forward(t):
        hidden_all(t)
        states = jnp.concatenate(
            [h[t, 0].reshape(3072, 128), h[t, 1].reshape(3072, 128)], axis=1)
        logits = jnp.dot(wt[...], states, preferred_element_type=F32)
        peak = jnp.max(logits, axis=0, keepdims=True)
        shifted = jnp.exp(logits - peak)
        hits = rows_of(f) == wanted(t)
        stx[t, f, 0:1, :] = peak
        stx[t, f, 1:2, :] = jnp.sum(shifted, axis=0, keepdims=True)
        stx[t, f, 2:3, :] = jnp.sum(jnp.where(hits, logits, 0.0), axis=0, keepdims=True)
        e[t, f] = shifted.astype(BF16)
        for k in range(1, 8):
            g = lax.rem(f + k, 8)
            send(stx.at[t, f], stx.at[t, f], sx_s.at[t, k], sx_r.at[t, f], at_f(g))
        block = e.at[t, f]
        send(block, block, e_s.at[t, 0], e_r.at[t, f], at_f(fp))
        send(block, block, e_s.at[t, 1], e_r.at[t, f], at_f(fm))
        send(block, block, e_s.at[t, 2], e_r.at[t, f], at_f(fq))

    def errors_2(t):
        arrived(e.at[t, fm], e_r.at[t, fm])
        block = e.at[t, fm, 0:128]
        send(block, block, e_s.at[t, 3], eh_r.at[t, 0], at_f(fp))
        arrived(e.at[t, fp], e_r.at[t, fp])
        block = e.at[t, fp, 128:256]
        send(block, block, e_s.at[t, 4], eh_r.at[t, 1], at_f(fm))
        for i, g in enumerate((fm, fp)):
            send(e.at[t, g], e.at[t, g], e_s.at[t, 5 + i], e_r.at[t, g], at_f(fq))

    def errors_3(t):
        arrived(e.at[t, fo, 0:128], eh_r.at[t, 0])
        arrived(e.at[t, fo, 128:256], eh_r.at[t, 1])
        send(e.at[t, fo], e.at[t, fo], e_s.at[t, 7], e_r.at[t, fo], at_f(fq))

    def combine(ref, t, n):
        peaks = [ref[t, i, 0:1, :] for i in range(n)]
        peak = functools.reduce(jnp.maximum, peaks)
        total = sum(ref[t, i, 1:2, :] * jnp.exp(peaks[i] - peak) for i in range(n))
        target = sum(ref[t, i, 2:3, :] for i in range(n))
        return peak, total, target

    def put(ref, t, i, values):
        for row, value in enumerate(values):
            ref[t, i, row:row + 1, :] = value

    def stats_y(t):
        for k in range(1, 8):
            g = lax.rem(f + k, 8)
            arrived(stx.at[t, g], sx_r.at[t, g])
        put(sty, t, y, combine(stx, t, 8))
        for k in range(1, Y):
            send(sty.at[t, y], sty.at[t, y], sy_s.at[t, k], sy_r.at[t, k], at_yz(lax.rem(y + k, Y), z))

    def stats_z(t):
        for k in range(1, Y):
            arrived(sty.at[t, lax.rem(y + Y - k, Y)], sy_r.at[t, k])
        put(stz, t, z, combine(sty, t, Y))
        for k in range(1, Z):
            send(stz.at[t, z], stz.at[t, z], sz_s.at[t, k], sz_r.at[t, k], at_yz(y, lax.rem(z + k, Z)))

    def backward(t):
        for k in range(1, Z):
            arrived(stz.at[t, lax.rem(z + Z - k, Z)], sz_r.at[t, k])
        peak, total, target = combine(stz, t, Z)
        full[t, 0:1, :] = jnp.log(total) + peak - target
        at_label = jnp.exp(target - peak) / total - 1.0
        for a in range(X):
            g = 2 * a + 1 - c
            arrived(e.at[t, g], e_r.at[t, g])
        for g in range(8):
            scale = jnp.exp(stx[t, g, 0:1, :] - peak) / total
            value = e[t, g].astype(F32) * scale
            value = jnp.where(rows_of(g) == wanted(t), at_label, value)
            errs[g, :, 256 * t:256 * t + 256] = value.astype(BF16)
        terms = jnp.dot(w[...], errs[:, :, 256 * t:256 * t + 256].reshape(2048, 256),
                        preferred_element_type=F32)
        sb[t] = terms.reshape(4, 96, 256)
        for k in range(1, Y):
            a = lax.rem(y + k, Y)
            send(sb.at[t, a], ry.at[t, k - 1], ry_s.at[t, k - 1], ry_r.at[t, k - 1], at_yz(a, z))

    def reduce_y(t):
        total = sb[t, y]
        for k in range(Y - 1):
            arrived(ry.at[t, k], ry_r.at[t, k])
            total = total + ry[t, k]
        for d in range(2):
            for r in range(4):
                zs[t, 4 * d + r] = total[24 * r:24 * r + 24, 128 * d:128 * d + 128]
        for k in range(1, Z):
            b = lax.rem(z + k, Z)
            send(zs.at[t, b], rz.at[t, k - 1], rz_s.at[t, k - 1], rz_r.at[t, k - 1], at_yz(y, b))

    def home_copy(t):
        return pltpu.make_async_remote_copy(
            src_ref=fs.at[t], dst_ref=fin.at[lax.rem(z, 4)], send_sem=f_s.at[t], recv_sem=f_r.at[lax.rem(z, 4)],
            device_id=home(t), device_id_type=pl.DeviceIdType.MESH)

    def reduce_z(t):
        total = zs[t, z]
        for k in range(Z - 1):
            arrived(rz.at[t, k], rz_r.at[t, k])
            total = total + rz[t, k]
        fs[t] = total
        stays = jnp.logical_and(own_home, x == t)

        @pl.when(stays)
        def _():
            fin[lax.rem(z, 4)] = fs[t]

        @pl.when(jnp.logical_not(stays))
        def _():
            home_copy(t).start()

    forward(0)
    hidden_y(3)
    hidden_end(1)
    forward(1)
    stats_y(0)
    errors_2(0)
    hidden_y2(2)
    hidden_end(2)
    forward(2)
    stats_y(1)
    stats_z(0)
    errors_2(1)
    errors_3(0)
    hidden_y2(3)
    hidden_end(3)
    forward(3)
    stats_y(2)
    stats_z(1)
    errors_2(2)
    errors_3(1)
    backward(0)
    stats_y(3)
    stats_z(2)
    errors_2(3)
    errors_3(2)
    backward(1)
    reduce_y(0)
    stats_z(3)
    errors_3(3)
    backward(2)
    reduce_y(1)
    reduce_z(0)
    backward(3)

    for t in range(X):
        for d in range(2):
            hs[:, 256 * t + 128 * d:256 * t + 128 * d + 128] = h[t, d, x, pl.ds(4 * c, 4)].reshape(384, 128)
    writes = []
    for g in range(8):
        gv[g] = lax.dot_general(hs[...], errs[g], (((1,), (1,)), ((), ())), preferred_element_type=F32)
        write = pltpu.make_async_copy(gv.at[g], grad_out.at[:, 256 * g:256 * g + 256], g_s.at[1 + g])
        write.start()
        writes.append(write)
        if g == 1:
            reduce_y(2)
        if g == 3:
            reduce_z(1)
    reduce_y(3)
    reduce_z(2)
    losses = full[x, 0:1, :]
    loss_out[...] = jnp.where(c == 0, losses[:, 0:128], losses[:, 128:256])
    reduce_z(3)
    for r in range(4):
        @pl.when(jnp.logical_not(jnp.logical_and(own_home, y == r)))
        def _():
            arrived(fin.at[r], f_r.at[r])
    spad[...] = jnp.zeros_like(spad)
    for r in range(4):
        spad[24 * r:24 * r + 24, :] = fin[r]
    state_out[...] = spad[...].T[:, 0:96].astype(BF16)
    for copy in sends:
        copy.wait_send()
    for t in range(X):
        @pl.when(jnp.logical_not(jnp.logical_and(own_home, x == t)))
        def _():
            home_copy(t).wait_send()
    for write in writes:
        write.wait()


def local(hidden_states, head, labels):
    dma = pltpu.SemaphoreType.DMA
    vmem = pltpu.VMEM
    loss, state, grad = pl.pallas_call(
        kernel,
        name="head_loss",
        out_shape=(
            jax.ShapeDtypeStruct((1, 128), F32),
            jax.ShapeDtypeStruct((128, 96), BF16),
            jax.ShapeDtypeStruct((384, 2048), F32),
        ),
        in_specs=[
            pl.BlockSpec(memory_space=vmem),
            pl.BlockSpec(memory_space=pl.ANY),
            pl.BlockSpec(memory_space=vmem),
        ],
        out_specs=(
            pl.BlockSpec(memory_space=vmem),
            pl.BlockSpec(memory_space=vmem),
            pl.BlockSpec(memory_space=pl.ANY),
        ),
        scratch_shapes=[
            vmem((384, 2048), BF16),
            vmem((8, 384, 256), BF16),
            vmem((2, 2, 192, 256), BF16),
            vmem((256, 3072), BF16),
            vmem((X, 2, Y, Z, 96, 128), BF16),
            vmem((128, 128), F32),
            vmem((8, 8, 128), jnp.int32),
            vmem((X, 8, 256, 256), BF16),
            vmem((8, 256, 1024), BF16),
            vmem((384, 1024), BF16),
            vmem((8, 384, 256), F32),
            vmem((X, 8, 8, 256), F32),
            vmem((X, Y, 8, 256), F32),
            vmem((X, Z, 8, 256), F32),
            vmem((X, 8, 256), F32),
            vmem((X, 4, 96, 256), F32),
            vmem((X, Y - 1, 96, 256), F32),
            vmem((X, Z, 24, 128), F32),
            vmem((X, Z - 1, 24, 128), F32),
            vmem((X, 24, 128), F32),
            vmem((4, 24, 128), F32),
            vmem((128, 128), F32),
            dma((2,)), dma((13,)), dma((8,)), dma((2, 2)), dma((2, 2)),
            dma((3,)), dma((X,)), dma((8,)), dma((8,)),
            dma((X, Z)), dma((X, Z)), dma((X, 4)), dma((X, 4)), dma((X, 4)), dma((X, 4)),
            dma((X, 8)), dma((X, 8)), dma((X, 2)),
            dma((X, 8)), dma((X, 8)), dma((X, Y)), dma((X, Y)), dma((X, Z)), dma((X, Z)),
            dma((X, Y - 1)), dma((X, Y - 1)), dma((X, Z - 1)), dma((X, Z - 1)),
            dma((X,)), dma((4,)), dma((9,)),
        ],
        compiler_params=pltpu.CompilerParams(
            collective_id=0, has_side_effects=True, vmem_limit_bytes=60 * 1024 * 1024),
    )(hidden_states, head, labels.reshape(1, 128))
    return (loss.reshape(128), state, grad)


def solution(mesh):
    in_specs = (P("fsdp", "vocab"), P("fsdp", "vocab"), P("fsdp"))
    out_specs = (P("fsdp"), P("fsdp", "vocab"), P("fsdp", "vocab"))
    return jax.shard_map(local, mesh=mesh, in_specs=in_specs, out_specs=out_specs, check_vma=False)
```

```python
import functools

import jax
import jax.numpy as jnp
from jax import lax
from jax.experimental import pallas as pl
from jax.experimental.pallas import tpu as pltpu
from jax.sharding import PartitionSpec as P

X, Y, Z = 4, 4, 8
LIMIT = 44
R = 2
F32, BF16 = jnp.float32, jnp.bfloat16


def kernel(hid, head, labels, loss_out, state_out, grad_out,
           w, wl, relay, wt, h, lab, e, errs, hs,
           stx, sty, stz, full, sb, ry, zs, rz, fs, fin,
           load_s, w_s, wl_r, rel_r, w2_r, b1_s, b1_r, lab_s, lab_r,
           hz_s, hz_r, hy_s, hy_r, hd_s, hd_r, hr_s, hr_r, rd_s, rd_r, e_s, e_r, eh_r,
           sx_s, sx_r, sy_s, sy_r, sz_s, sz_r,
           ry_s, ry_r, rz_s, rz_r, f_s, f_r, g_s):
    f, v = lax.axis_index("fsdp"), lax.axis_index("vocab")
    x, c = lax.div(f, 2), lax.rem(f, 2)
    y, z = lax.div(v, Z), lax.rem(v, Z)
    xp, xm, xo = lax.rem(x + 1, X), lax.rem(x + 3, X), lax.rem(x + 2, X)
    yp, ym, yo = lax.rem(y + 1, Y), lax.rem(y + 3, Y), lax.rem(y + 2, Y)
    fp, fm, fo, fq = 2 * xp + c, 2 * xm + c, 2 * xo + c, 2 * x + 1 - c
    sends = []

    def at_f(g):
        return {"fsdp": g, "vocab": v}

    def at_yz(a, b):
        return {"fsdp": f, "vocab": Z * a + b}

    def send(src, dst, ssem, rsem, device):
        copy = pltpu.make_async_remote_copy(
            src_ref=src, dst_ref=dst, send_sem=ssem, recv_sem=rsem,
            device_id=device, device_id_type=pl.DeviceIdType.MESH)
        copy.start()
        sends.append(copy)

    def arrived(dst, rsem):
        pltpu.make_async_remote_copy(
            src_ref=dst, dst_ref=dst, send_sem=g_s.at[0], recv_sem=rsem,
            device_id=at_f(fq), device_id_type=pl.DeviceIdType.MESH).wait_recv()

    def home(t):
        return {"fsdp": 2 * t + lax.div(z, 4), "vocab": Z * x + 4 * c + y}

    def origin(r):
        return {"fsdp": 2 * y + lax.div(z, 4), "vocab": Z * lax.rem(z, 4) + 4 * c + r}

    own_home = jnp.logical_and(y == x, z == 4 * c + y)

    load_w = pltpu.make_async_copy(head, w, load_s.at[0])
    load_w.start()
    columns = pl.ds(pl.multiple_of(256 * f, 256), 256)
    load_own = pltpu.make_async_copy(head.at[:, columns], wl.at[f], load_s.at[1])
    load_own.start()

    barrier = pltpu.get_barrier_semaphore()

    def hello(device):
        pl.semaphore_signal(barrier, inc=1, device_id=device, device_id_type=pl.DeviceIdType.MESH)

    for k in range(1, 8):
        hello(at_f(lax.rem(f + k, 8)))
    for k in range(1, Y):
        hello(at_yz(lax.rem(y + k, Y), z))
    for k in range(1, Z):
        hello(at_yz(y, lax.rem(z + k, Z)))
    for r in range(4):
        @pl.when(jnp.logical_not(jnp.logical_and(own_home, y == r)))
        def _():
            hello(origin(r))

    load_hid = pltpu.make_async_copy(hid, h.at[x, c, y, z], load_s.at[2])
    load_hid.start()
    load_lab = pltpu.make_async_copy(labels, lab.at[f, 0:1], load_s.at[3])
    load_lab.start()

    def begin():
        load_w.wait()
        load_hid.wait()
        load_lab.wait()
        pl.semaphore_wait(barrier, 7 + 3 + 7 + 4 - own_home.astype(jnp.int32))

    begin()

    mine = h.at[x, c, y, z]
    for i, g in enumerate((fp, fm, fo)):
        send(mine, mine, b1_s.at[i], b1_r.at[x], at_f(g))
    for k in range(1, 8):
        send(lab.at[f], lab.at[f], lab_s.at[k], lab_r.at[f], at_f(lax.rem(f + k, 8)))

    def cols(g):
        return pl.ds(pl.multiple_of(256 * g, 256), 256)

    for d in range(2):
        send(w.at[0:192, cols(2 * xo + d)], relay.at[0, d], w_s.at[d], rel_r.at[0, d], at_f(fp))
        send(w.at[192:384, cols(2 * xo + d)], relay.at[1, d], w_s.at[2 + d], rel_r.at[1, d], at_f(fm))
    send(w.at[:, cols(fq)], wl.at[f], w_s.at[4], wl_r.at[f], at_f(fq))
    for d in range(2):
        send(w.at[:, cols(2 * xp + d)], wl.at[f], w_s.at[5 + d], wl_r.at[f], at_f(2 * xp + d))
        send(w.at[:, cols(2 * xm + d)], wl.at[f], w_s.at[7 + d], wl_r.at[f], at_f(2 * xm + d))

    def hidden_z(t):
        block = h.at[t, c, y, z]

        @pl.when(x != t)
        def _():
            arrived(block, b1_r.at[t])

        for k in range(1, Z):
            send(block, block, hz_s.at[t, k], hz_r.at[t, k], at_yz(y, lax.rem(z + k, Z)))

    def ring_y():
        block = h.at[R, c, y, z]

        @pl.when(x != R)
        def _():
            arrived(block, b1_r.at[R])

        for k in range(1, Y):
            send(block, block, hz_s.at[R, k], hz_r.at[R, k], at_yz(lax.rem(y + k, Y), z))

    zp, zm = lax.rem(z + 1, Z), lax.rem(z + Z - 1, Z)

    def ring_send(step):
        right = lax.rem(z + Z + 1 - step, Z)
        left = lax.rem(z + step - 1, Z)
        low, high = ((0, 4), (0, 4)) if step < 4 else ((0, 2), (2, 4))
        block = h.at[R, c, low[0]:low[1], right]
        send(block, block, hr_s.at[0, step], hr_r.at[0, step], at_yz(y, zp))
        block = h.at[R, c, high[0]:high[1], left]
        send(block, block, hr_s.at[1, step], hr_r.at[1, step], at_yz(y, zm))

    def ring_partner(n, column):
        block = h.at[R, c, :, column]
        send(block, block, rd_s.at[n], rd_r.at[n], at_f(fq))

    def ring_start():
        for k in range(1, Y):
            arrived(h.at[R, c, lax.rem(y + Y - k, Y), z], hz_r.at[R, k])
        ring_send(1)
        ring_partner(0, z)

    def ring_next(step):
        left, right = lax.rem(z + Z - step, Z), lax.rem(z + step, Z)
        arrived(h.at[R, c, :, left], hr_r.at[0, step])
        arrived(h.at[R, c, :, right], hr_r.at[1, step])
        ring_send(step + 1)
        ring_partner(2 * step - 1, left)
        ring_partner(2 * step, right)

    def ring_end():
        far = lax.rem(z + 4, Z)
        arrived(h.at[R, c, 0:2, far], hr_r.at[0, 4])
        arrived(h.at[R, c, 2:4, far], hr_r.at[1, 4])
        ring_partner(7, far)


    def relays():
        for d in range(2):
            arrived(relay.at[0, d], rel_r.at[0, d])
            send(relay.at[0, d], wl.at[fm, 0:192], w_s.at[9 + d], w2_r.at[0, c], at_f(2 * xp + d))
            arrived(relay.at[1, d], rel_r.at[1, d])
            send(relay.at[1, d], wl.at[fp, 192:384], w_s.at[11 + d], w2_r.at[1, c], at_f(2 * xm + d))


    def to_partner(t, row, n):
        block = h.at[t, c, row]
        send(block, block, hd_s.at[t, n], hd_r.at[t, n], at_f(fq))

    def hidden_y(t):
        for k in range(1, Z):
            arrived(h.at[t, c, y, lax.rem(z + Z - k, Z)], hz_r.at[t, k])
        low, high = h.at[t, c, y, 0:4], h.at[t, c, y, 4:8]
        send(low, low, hy_s.at[t, 0], hy_r.at[t, 0], at_yz(yp, z))
        send(high, high, hy_s.at[t, 1], hy_r.at[t, 1], at_yz(ym, z))
        send(high, high, hy_s.at[t, 4], hy_r.at[t, 4], at_yz(yp, z))
        send(low, low, hy_s.at[t, 5], hy_r.at[t, 5], at_yz(ym, z))
        to_partner(t, y, 0)

    def hidden_y2(t):
        block = h.at[t, c, ym, 0:4]
        arrived(block, hy_r.at[t, 0])
        send(block, block, hy_s.at[t, 2], hy_r.at[t, 2], at_yz(yp, z))
        block = h.at[t, c, yp, 4:8]
        arrived(block, hy_r.at[t, 1])
        send(block, block, hy_s.at[t, 3], hy_r.at[t, 3], at_yz(ym, z))

    def hidden_end(t):
        arrived(h.at[t, c, ym, 4:8], hy_r.at[t, 4])
        arrived(h.at[t, c, yp, 0:4], hy_r.at[t, 5])
        to_partner(t, ym, 1)
        to_partner(t, yp, 2)
        arrived(h.at[t, c, yo, 0:4], hy_r.at[t, 2])
        arrived(h.at[t, c, yo, 4:8], hy_r.at[t, 3])
        to_partner(t, yo, 3)

    def hidden_all(t):
        if t == R:
            for n, k in enumerate((0, 7, 1, 6, 2, 5, 3, 4)):
                arrived(h.at[t, 1 - c, :, lax.rem(z + k, Z)], rd_r.at[n])
        else:
            for n, row in enumerate((y, ym, yp, yo)):
                arrived(h.at[t, 1 - c, row], hd_r.at[t, n])

    def head_in():
        load_own.wait()
        for g in (fq, 2 * xp, 2 * xp + 1, 2 * xm, 2 * xm + 1):
            arrived(wl.at[g], wl_r.at[g])
        for d in range(2):
            arrived(wl.at[2 * xo + d, 0:192], w2_r.at[0, d])
            arrived(wl.at[2 * xo + d, 192:384], w2_r.at[1, d])

    hidden_z(0)
    hidden_z(1)
    hidden_z(3)
    ring_y()
    ring_start()
    relays()
    hidden_y(0)
    hidden_y2(0)
    hidden_y(1)
    ring_next(1)
    head_in()
    for g in range(8):
        wt[:, 384 * g:384 * g + 384] = wl[g].T
    for k in range(1, 8):
        g = lax.rem(f + k, 8)
        arrived(lab.at[g], lab_r.at[g])

    def wanted(t):
        return jnp.concatenate([lab[2 * t, 0:1, :], lab[2 * t + 1, 0:1, :]], axis=1)

    def rows_of(g):
        return v * 2048 + g * 256 + lax.broadcasted_iota(jnp.int32, (256, 256), 0)

    def forward(t):
        hidden_all(t)
        states = jnp.concatenate(
            [h[t, 0].reshape(3072, 128), h[t, 1].reshape(3072, 128)], axis=1)
        logits = jnp.dot(wt[...], states, preferred_element_type=F32)
        peak = jnp.max(logits, axis=0, keepdims=True)
        shifted = jnp.exp(logits - peak)
        hits = rows_of(f) == wanted(t)
        stx[t, f, 0:1, :] = peak
        stx[t, f, 1:2, :] = jnp.sum(shifted, axis=0, keepdims=True)
        stx[t, f, 2:3, :] = jnp.sum(jnp.where(hits, logits, 0.0), axis=0, keepdims=True)
        e[t, f] = shifted.astype(BF16)
        for k in range(1, 8):
            g = lax.rem(f + k, 8)
            send(stx.at[t, f], stx.at[t, f], sx_s.at[t, k], sx_r.at[t, f], at_f(g))
        low, high, block = e.at[t, f, 0:128], e.at[t, f, 128:256], e.at[t, f]
        send(low, low, e_s.at[t, 0], eh_r.at[t, 2], at_f(fp))
        send(high, high, e_s.at[t, 1], eh_r.at[t, 3], at_f(fm))
        send(high, high, e_s.at[t, 8], eh_r.at[t, 4], at_f(fp))
        send(low, low, e_s.at[t, 9], eh_r.at[t, 5], at_f(fm))
        send(block, block, e_s.at[t, 2], e_r.at[t, f], at_f(fq))

    def errors_2(t):
        block = e.at[t, fm, 0:128]
        arrived(block, eh_r.at[t, 2])
        send(block, block, e_s.at[t, 3], eh_r.at[t, 0], at_f(fp))
        block = e.at[t, fp, 128:256]
        arrived(block, eh_r.at[t, 3])
        send(block, block, e_s.at[t, 4], eh_r.at[t, 1], at_f(fm))

    def errors_3(t):
        arrived(e.at[t, fm, 128:256], eh_r.at[t, 4])
        arrived(e.at[t, fp, 0:128], eh_r.at[t, 5])
        for i, g in enumerate((fm, fp)):
            send(e.at[t, g], e.at[t, g], e_s.at[t, 5 + i], e_r.at[t, g], at_f(fq))
        arrived(e.at[t, fo, 0:128], eh_r.at[t, 0])
        arrived(e.at[t, fo, 128:256], eh_r.at[t, 1])
        send(e.at[t, fo], e.at[t, fo], e_s.at[t, 7], e_r.at[t, fo], at_f(fq))

    def combine(ref, t, n):
        peaks = [ref[t, i, 0:1, :] for i in range(n)]
        peak = functools.reduce(jnp.maximum, peaks)
        total = sum(ref[t, i, 1:2, :] * jnp.exp(peaks[i] - peak) for i in range(n))
        target = sum(ref[t, i, 2:3, :] for i in range(n))
        return peak, total, target

    def put(ref, t, i, values):
        for row, value in enumerate(values):
            ref[t, i, row:row + 1, :] = value

    def stats_y(t):
        for k in range(1, 8):
            g = lax.rem(f + k, 8)
            arrived(stx.at[t, g], sx_r.at[t, g])
        put(sty, t, y, combine(stx, t, 8))
        for k in range(1, Y):
            send(sty.at[t, y], sty.at[t, y], sy_s.at[t, k], sy_r.at[t, k], at_yz(lax.rem(y + k, Y), z))

    def stats_z(t):
        for k in range(1, Y):
            arrived(sty.at[t, lax.rem(y + Y - k, Y)], sy_r.at[t, k])
        put(stz, t, z, combine(sty, t, Y))
        for k in range(1, Z):
            send(stz.at[t, z], stz.at[t, z], sz_s.at[t, k], sz_r.at[t, k], at_yz(y, lax.rem(z + k, Z)))

    def backward(t):
        for k in range(1, Z):
            arrived(stz.at[t, lax.rem(z + Z - k, Z)], sz_r.at[t, k])
        peak, total, target = combine(stz, t, Z)
        full[t, 0:1, :] = jnp.log(total) + peak - target
        at_label = jnp.exp(target - peak) / total - 1.0
        for a in range(X):
            g = 2 * a + 1 - c
            arrived(e.at[t, g], e_r.at[t, g])
        for g in range(8):
            scale = jnp.exp(stx[t, g, 0:1, :] - peak) / total
            value = e[t, g].astype(F32) * scale
            value = jnp.where(rows_of(g) == wanted(t), at_label, value)
            errs[g, :, 256 * t:256 * t + 256] = value.astype(BF16)
        terms = jnp.dot(w[...], errs[:, :, 256 * t:256 * t + 256].reshape(2048, 256),
                        preferred_element_type=F32)
        sb[t] = terms.reshape(4, 96, 256)
        for k in range(1, Y):
            a = lax.rem(y + k, Y)
            send(sb.at[t, a], ry.at[t, k - 1], ry_s.at[t, k - 1], ry_r.at[t, k - 1], at_yz(a, z))

    def reduce_y(t):
        total = sb[t, y]
        for k in range(Y - 1):
            arrived(ry.at[t, k], ry_r.at[t, k])
            total = total + ry[t, k]
        for d in range(2):
            for r in range(4):
                zs[t, 4 * d + r] = total[24 * r:24 * r + 24, 128 * d:128 * d + 128]
        for k in range(1, Z):
            b = lax.rem(z + k, Z)
            send(zs.at[t, b], rz.at[t, k - 1], rz_s.at[t, k - 1], rz_r.at[t, k - 1], at_yz(y, b))

    def home_copy(t):
        return pltpu.make_async_remote_copy(
            src_ref=fs.at[t], dst_ref=fin.at[lax.rem(z, 4)], send_sem=f_s.at[t], recv_sem=f_r.at[lax.rem(z, 4)],
            device_id=home(t), device_id_type=pl.DeviceIdType.MESH)

    def reduce_z(t):
        total = zs[t, z]
        for k in range(Z - 1):
            arrived(rz.at[t, k], rz_r.at[t, k])
            total = total + rz[t, k]
        fs[t] = total
        stays = jnp.logical_and(own_home, x == t)

        @pl.when(stays)
        def _():
            fin[lax.rem(z, 4)] = fs[t]

        @pl.when(jnp.logical_not(stays))
        def _():
            home_copy(t).start()

    hidden_end(0)
    forward(0)
    hidden_y2(1)
    hidden_y(3)
    ring_next(2)
    hidden_end(1)
    forward(1)
    errors_2(0)
    ring_next(3)
    hidden_y2(3)
    stats_y(0)
    ring_end()
    forward(2)
    errors_2(1)
    errors_3(0)
    stats_y(1)
    stats_z(0)
    hidden_end(3)
    forward(3)
    errors_2(2)
    errors_3(1)
    stats_y(2)
    stats_z(1)
    stats_y(3)
    backward(0)
    errors_2(3)
    stats_z(2)
    errors_3(2)
    stats_z(3)
    backward(1)
    errors_3(3)
    backward(2)
    reduce_y(0)
    backward(3)
    reduce_y(1)
    reduce_z(0)

    for t in range(X):
        for d in range(2):
            hs[:, 256 * t + 128 * d:256 * t + 128 * d + 128] = h[t, d, x, pl.ds(4 * c, 4)].reshape(384, 128)
    for g in range(8):
        grad_out[:, 256 * g:256 * g + 256] = lax.dot_general(
            hs[...], errs[g], (((1,), (1,)), ((), ())), preferred_element_type=F32)
        if g == 1:
            reduce_y(2)
        if g == 3:
            reduce_z(1)
    reduce_y(3)
    reduce_z(2)
    losses = full[x, 0:1, :]
    loss_out[...] = jnp.where(c == 0, losses[:, 0:128], losses[:, 128:256])
    reduce_z(3)
    for r in range(4):
        @pl.when(jnp.logical_not(jnp.logical_and(own_home, y == r)))
        def _():
            arrived(fin.at[r], f_r.at[r])
    state_out[...] = fin[...].reshape(96, 128).astype(BF16)

    def drain():
        for copy in sends:
            copy.wait_send()
        for t in range(X):
            @pl.when(jnp.logical_not(jnp.logical_and(own_home, x == t)))
            def _():
                home_copy(t).wait_send()

    drain()


def local(hidden_states, head, labels):
    dma = pltpu.SemaphoreType.DMA
    vmem = pltpu.VMEM
    loss, state, grad = pl.pallas_call(
        kernel,
        name="head_loss",
        out_shape=(
            jax.ShapeDtypeStruct((1, 128), F32),
            jax.ShapeDtypeStruct((96, 128), BF16),
            jax.ShapeDtypeStruct((384, 2048), F32),
        ),
        in_specs=[pl.BlockSpec(memory_space=pltpu.HBM)] * 3,
        out_specs=(
            pl.BlockSpec(memory_space=vmem),
            pl.BlockSpec(memory_space=vmem),
            pl.BlockSpec(memory_space=vmem),
        ),
        scratch_shapes=[
            vmem((384, 2048), BF16),
            vmem((8, 384, 256), BF16),
            vmem((2, 2, 192, 256), BF16),
            vmem((256, 3072), BF16),
            vmem((X, 2, Y, Z, 96, 128), BF16),
            vmem((8, 8, 128), jnp.int32),
            vmem((X, 8, 256, 256), BF16),
            vmem((8, 256, 1024), BF16),
            vmem((384, 1024), BF16),
            vmem((X, 8, 8, 256), F32),
            vmem((X, Y, 8, 256), F32),
            vmem((X, Z, 8, 256), F32),
            vmem((X, 8, 256), F32),
            vmem((X, 4, 96, 256), F32),
            vmem((X, Y - 1, 96, 256), F32),
            vmem((X, Z, 24, 128), F32),
            vmem((X, Z - 1, 24, 128), F32),
            vmem((X, 24, 128), F32),
            vmem((4, 24, 128), F32),
            dma((4,)), dma((13,)), dma((8,)), dma((2, 2)), dma((2, 2)),
            dma((3,)), dma((X,)), dma((8,)), dma((8,)),
            dma((X, Z)), dma((X, Z)), dma((X, 6)), dma((X, 6)), dma((X, 4)), dma((X, 4)),
            dma((2, 5)), dma((2, 5)), dma((8,)), dma((8,)),
            dma((X, 10)), dma((X, 8)), dma((X, 6)),
            dma((X, 8)), dma((X, 8)), dma((X, Y)), dma((X, Y)), dma((X, Z)), dma((X, Z)),
            dma((X, Y - 1)), dma((X, Y - 1)), dma((X, Z - 1)), dma((X, Z - 1)),
            dma((X,)), dma((4,)), dma((1,)),
        ],
        compiler_params=pltpu.CompilerParams(
            collective_id=0, has_side_effects=True, vmem_limit_bytes=LIMIT * 1024 * 1024),
    )(*(pltpu.with_memory_space_constraint(a, pltpu.HBM)
        for a in (hidden_states.T, head, labels.reshape(1, 128))))
    return (loss.reshape(128), state.T, grad)


def solution(mesh):
    in_specs = (P("fsdp", "vocab"), P("fsdp", "vocab"), P("fsdp"))
    out_specs = (P("fsdp"), P("fsdp", "vocab"), P("fsdp", "vocab"))
    return jax.shard_map(local, mesh=mesh, in_specs=in_specs, out_specs=out_specs, check_vma=False)
```

```python
import functools

import jax
import jax.numpy as jnp
from jax import lax
from jax.experimental import pallas as pl
from jax.experimental.pallas import tpu as pltpu
from jax.sharding import PartitionSpec as P

X, Y, Z = 4, 4, 8
LIMIT = 44
R = 2
HALVES = ((0, 0), (1, 4), (0, 4), (1, 0), (2, 0), (2, 4))
F32, BF16 = jnp.float32, jnp.bfloat16


def kernel(hid, head, labels, loss_out, state_out, grad_out,
           w, wl, relay, wt, h, own, lab, e, errs, hs,
           stx, sty, stz, full, sb, ry, zs, rz, fs, fin,
           load_s, w_s, wl_r, rel_r, w2_r, b1_s, b1_r, lab_s, lab_r,
           hz_s, hz_r, hy_s, hy_r, hd_s, hd_r, hr_s, hr_r, rd_s, rd_r, e_s, e_r, eh_r,
           sx_s, sx_r, sy_s, sy_r, sz_s, sz_r,
           ry_s, ry_r, rz_s, rz_r, f_s, f_r, g_s):
    f, v = lax.axis_index("fsdp"), lax.axis_index("vocab")
    x, c = lax.div(f, 2), lax.rem(f, 2)
    y, z = lax.div(v, Z), lax.rem(v, Z)
    xp, xm, xo = lax.rem(x + 1, X), lax.rem(x + 3, X), lax.rem(x + 2, X)
    yp, ym, yo = lax.rem(y + 1, Y), lax.rem(y + 3, Y), lax.rem(y + 2, Y)
    fp, fm, fo, fq = 2 * xp + c, 2 * xm + c, 2 * xo + c, 2 * x + 1 - c
    ys = [lax.rem(y + k, Y) for k in range(Y)]
    zs_at = [lax.rem(z + k, Z) for k in range(Z)]
    xs = [x, xp, xo, xm]
    group = [[2 * a + d for d in range(2)] for a in xs]
    to_y = [{"fsdp": f, "vocab": Z * a + z} for a in ys]
    to_z = [{"fsdp": f, "vocab": Z * y + b} for b in zs_at]
    sends, calls, draining = [], {0: [], 1: []}, [False]
    role = [None]

    def only(core):
        def wrap(fn):
            def run(*args):
                calls[core].append((fn, args))

                @pl.when(c == core)
                def _():
                    role[0] = core
                    fn(*args)
                    role[0] = None
            run.__name__ = fn.__name__
            return run
        return wrap

    def at_f(g):
        return {"fsdp": g, "vocab": v}

    partner = at_f(fq)

    def send(src, dst, ssem, rsem, device):
        copy = pltpu.make_async_remote_copy(
            src_ref=src, dst_ref=dst, send_sem=ssem, recv_sem=rsem,
            device_id=device, device_id_type=pl.DeviceIdType.MESH)
        if draining[0]:
            copy.wait_send()
            return
        copy.start()
        if role[0] is None:
            sends.append(copy)

    def arrived(dst, rsem):
        if draining[0]:
            return
        pltpu.make_async_remote_copy(
            src_ref=dst, dst_ref=dst, send_sem=g_s.at[0], recv_sem=rsem,
            device_id=partner, device_id_type=pl.DeviceIdType.MESH).wait_recv()

    def home(t):
        return {"fsdp": 2 * t + lax.div(z, 4), "vocab": Z * x + 4 * c + y}

    def origin(r):
        return {"fsdp": 2 * y + lax.div(z, 4), "vocab": Z * lax.rem(z, 4) + 4 * c + r}

    own_home = jnp.logical_and(y == x, z == 4 * c + y)

    load_w = pltpu.make_async_copy(head, w, load_s.at[0])
    load_w.start()
    columns = pl.ds(pl.multiple_of(256 * f, 256), 256)
    load_own = pltpu.make_async_copy(head.at[:, columns], wl.at[f], load_s.at[1])
    load_own.start()

    barrier = pltpu.get_barrier_semaphore()

    def hello(device):
        pl.semaphore_signal(barrier, inc=1, device_id=device, device_id_type=pl.DeviceIdType.MESH)

    for k in range(1, 8):
        hello(at_f(lax.rem(f + k, 8)))
    for k in range(1, Y):
        hello(to_y[k])
    for k in range(1, Z):
        hello(to_z[k])
    for r in range(4):
        @pl.when(jnp.logical_not(jnp.logical_and(own_home, y == r)))
        def _():
            hello(origin(r))

    load_hid = pltpu.make_async_copy(hid, own, load_s.at[2])
    load_hid.start()
    load_lab = pltpu.make_async_copy(labels, lab.at[f, 0:1], load_s.at[3])
    load_lab.start()
    load_mine = pltpu.make_async_copy(hid, h.at[x, y, z, 1], load_s.at[4])

    @pl.when(c == 1)
    def _():
        load_mine.start()

    def begin():
        load_w.wait()
        load_hid.wait()
        load_lab.wait()

        @pl.when(c == 1)
        def _():
            load_mine.wait()

        pl.semaphore_wait(barrier, 7 + 3 + 7 + 4 - own_home.astype(jnp.int32))

    begin()

    for i in range(1, X):
        send(own, h.at[x, y, z, c], b1_s.at[i], b1_r.at[x, c], at_f(group[i][1]))

    def to_carrier():
        send(own, h.at[x, y, z, 0], b1_s.at[0], b1_r.at[x, 0], partner)

    to_carrier = only(0)(to_carrier)
    to_carrier()
    for k in range(1, 8):
        send(lab.at[f], lab.at[f], lab_s.at[k], lab_r.at[f], at_f(lax.rem(f + k, 8)))

    def cols(g):
        return pl.ds(pl.multiple_of(256 * g, 256), 256)

    for d in range(2):
        send(w.at[0:192, cols(2 * xo + d)], relay.at[0, c, d], w_s.at[d], rel_r.at[0, c, d], at_f(group[1][0]))
        send(w.at[192:384, cols(2 * xo + d)], relay.at[1, c, d], w_s.at[2 + d], rel_r.at[1, c, d], at_f(group[3][0]))
    send(w.at[:, cols(fq)], wl.at[f], w_s.at[4], wl_r.at[f], at_f(fq))
    for d in range(2):
        send(w.at[:, cols(2 * xp + d)], wl.at[f], w_s.at[5 + d], wl_r.at[f], at_f(2 * xp + d))
        send(w.at[:, cols(2 * xm + d)], wl.at[f], w_s.at[7 + d], wl_r.at[f], at_f(2 * xm + d))

    def head_in():
        load_own.wait()
        for g in (fq, 2 * xp, 2 * xp + 1, 2 * xm, 2 * xm + 1):
            arrived(wl.at[g], wl_r.at[g])
        for d in range(2):
            arrived(wl.at[2 * xo + d, 0:192], w2_r.at[0, d])
            arrived(wl.at[2 * xo + d, 192:384], w2_r.at[1, d])

    @only(0)
    def relays():
        for d in range(2):
            for o in range(2):
                arrived(relay.at[0, o, d], rel_r.at[0, o, d])
                send(relay.at[0, o, d], wl.at[group[3][o], 0:192],
                     w_s.at[9 + 2 * d + o], w2_r.at[0, o], at_f(group[1][d]))
                arrived(relay.at[1, o, d], rel_r.at[1, o, d])
                send(relay.at[1, o, d], wl.at[group[1][o], 192:384],
                     w_s.at[13 + 2 * d + o], w2_r.at[1, o], at_f(group[3][d]))

    def have(t):
        arrived(h.at[t, y, z, 0], b1_r.at[t, 0])

        @pl.when(x != t)
        def _():
            arrived(h.at[t, y, z, 1], b1_r.at[t, 1])

    @only(1)
    def hidden_z(t):
        have(t)
        block = h.at[t, y, z]
        for k in range(1, Z):
            send(block, block, hz_s.at[t, k], hz_r.at[t, k], to_z[k])

    @only(1)
    def ring_y():
        have(R)
        block = h.at[R, y, z]
        for k in range(1, Y):
            send(block, block, hz_s.at[R, k], hz_r.at[R, k], to_y[k])

    def ring_send(step):
        right, left = zs_at[(1 - step) % Z], zs_at[step - 1]
        low, high = ((0, 4), (0, 4)) if step < 4 else ((0, 2), (2, 4))
        block = h.at[R, low[0]:low[1], right]
        send(block, block, hr_s.at[0, step], hr_r.at[0, step], to_z[1])
        block = h.at[R, high[0]:high[1], left]
        send(block, block, hr_s.at[1, step], hr_r.at[1, step], to_z[7])

    def ring_partner(n, column):
        block = h.at[R, :, column]
        send(block, block, rd_s.at[n], rd_r.at[n], partner)

    @only(1)
    def ring_start():
        for k in range(1, Y):
            arrived(h.at[R, ys[Y - k], z], hz_r.at[R, k])
        ring_send(1)
        ring_partner(0, z)

    @only(1)
    def ring_next(step):
        left, right = zs_at[Z - step], zs_at[step]
        arrived(h.at[R, :, left], hr_r.at[0, step])
        arrived(h.at[R, :, right], hr_r.at[1, step])
        ring_send(step + 1)
        ring_partner(2 * step - 1, left)
        ring_partner(2 * step, right)

    @only(1)
    def ring_end():
        far = zs_at[4]
        arrived(h.at[R, 0:2, far], hr_r.at[0, 4])
        arrived(h.at[R, 2:4, far], hr_r.at[1, 4])
        ring_partner(7, far)

    def to_partner(t, row, low, n):
        block = h.at[t, row, low:low + (4 if n else Z)]
        send(block, block, hd_s.at[t, n], hd_r.at[t, n], partner)

    @only(1)
    def hidden_y(t):
        for k in range(1, Z):
            arrived(h.at[t, y, zs_at[Z - k]], hz_r.at[t, k])
        low, high = h.at[t, y, 0:4], h.at[t, y, 4:8]
        send(low, low, hy_s.at[t, 0], hy_r.at[t, 0], to_y[1])
        send(high, high, hy_s.at[t, 1], hy_r.at[t, 1], to_y[3])
        send(high, high, hy_s.at[t, 4], hy_r.at[t, 4], to_y[1])
        send(low, low, hy_s.at[t, 5], hy_r.at[t, 5], to_y[3])
        to_partner(t, y, 0, 0)

    @only(1)
    def hidden_y2(t):
        block = h.at[t, ym, 0:4]
        arrived(block, hy_r.at[t, 0])
        send(block, block, hy_s.at[t, 2], hy_r.at[t, 2], to_y[1])
        block = h.at[t, yp, 4:8]
        arrived(block, hy_r.at[t, 1])
        send(block, block, hy_s.at[t, 3], hy_r.at[t, 3], to_y[3])
        to_partner(t, ym, 0, 1)
        to_partner(t, yp, 4, 2)

    @only(1)
    def hidden_end(t):
        for n, (row, low) in enumerate(HALVES[2:]):
            row = (ym, yp, yo)[row]
            arrived(h.at[t, row, low:low + 4], hy_r.at[t, (4, 5, 2, 3)[n]])
            to_partner(t, row, low, 3 + n)

    @only(0)
    def hidden_all(t):
        if t == R:
            for n, k in enumerate((0, 7, 1, 6, 2, 5, 3, 4)):
                arrived(h.at[t, :, zs_at[k]], rd_r.at[n])
        else:
            arrived(h.at[t, y], hd_r.at[t, 0])
            for n, (row, low) in enumerate(HALVES):
                arrived(h.at[t, (ym, yp, yo)[row], low:low + 4], hd_r.at[t, 1 + n])

    hidden_z(0)
    hidden_z(3)
    hidden_z(1)
    ring_y()
    ring_start()
    hidden_y(0)
    relays()
    hidden_y2(0)
    hidden_y(3)
    ring_next(1)
    hidden_end(0)
    hidden_y2(3)
    hidden_y(1)
    head_in()
    for g in range(8):
        wt[:, 384 * g:384 * g + 384] = wl[g].T
    for k in range(1, 8):
        g = lax.rem(f + k, 8)
        arrived(lab.at[g], lab_r.at[g])

    def wanted(t):
        return jnp.concatenate([lab[2 * t, 0:1, :], lab[2 * t + 1, 0:1, :]], axis=1)

    def rows_of(g):
        return v * 2048 + g * 256 + lax.broadcasted_iota(jnp.int32, (256, 256), 0)

    def forward(t):
        hidden_all(t)
        states = jnp.concatenate(
            [h[t, :, :, 0].reshape(3072, 128), h[t, :, :, 1].reshape(3072, 128)], axis=1)
        logits = jnp.dot(wt[...], states, preferred_element_type=F32)
        peak = jnp.max(logits, axis=0, keepdims=True)
        shifted = jnp.exp(logits - peak)
        hits = rows_of(f) == wanted(t)
        stx[t, f, 0:1, :] = peak
        stx[t, f, 1:2, :] = jnp.sum(shifted, axis=0, keepdims=True)
        stx[t, f, 2:3, :] = jnp.sum(jnp.where(hits, logits, 0.0), axis=0, keepdims=True)
        e[t, f] = shifted.astype(BF16)
        for k in range(1, 8):
            g = lax.rem(f + k, 8)
            send(stx.at[t, f], stx.at[t, f], sx_s.at[t, k], sx_r.at[t, f], at_f(g))
        low, high, block = e.at[t, f, 0:128], e.at[t, f, 128:256], e.at[t, f]
        send(low, low, e_s.at[t, 0], eh_r.at[t, c, 2], at_f(group[1][0]))
        send(high, high, e_s.at[t, 1], eh_r.at[t, c, 3], at_f(group[3][0]))
        send(high, high, e_s.at[t, 2], eh_r.at[t, c, 4], at_f(group[1][0]))
        send(low, low, e_s.at[t, 3], eh_r.at[t, c, 5], at_f(group[3][0]))
        send(block, block, e_s.at[t, 4], e_r.at[t, f], partner)

    @only(0)
    def errors_2(t):
        for d in range(2):
            block = e.at[t, group[3][d], 0:128]
            arrived(block, eh_r.at[t, d, 2])
            send(block, block, e_s.at[t, 5 + d], eh_r.at[t, d, 0], at_f(group[1][0]))
            block = e.at[t, group[1][d], 128:256]
            arrived(block, eh_r.at[t, d, 3])
            send(block, block, e_s.at[t, 7 + d], eh_r.at[t, d, 1], at_f(group[3][0]))

    @only(0)
    def errors_3(t):
        for d in range(2):
            arrived(e.at[t, group[3][d], 128:256], eh_r.at[t, d, 4])
            arrived(e.at[t, group[1][d], 0:128], eh_r.at[t, d, 5])
            for i, a in enumerate((3, 1)):
                block = e.at[t, group[a][d]]
                send(block, block, e_s.at[t, 9 + 2 * d + i], e_r.at[t, group[a][d]], partner)
        for d in range(2):
            block = e.at[t, group[2][d]]
            arrived(e.at[t, group[2][d], 0:128], eh_r.at[t, d, 0])
            arrived(e.at[t, group[2][d], 128:256], eh_r.at[t, d, 1])
            send(block, block, e_s.at[t, 13 + d], e_r.at[t, group[2][d]], partner)

    @only(1)
    def errors_all(t):
        for a in (3, 1, 2):
            for d in range(2):
                arrived(e.at[t, group[a][d]], e_r.at[t, group[a][d]])

    def combine(ref, t, n):
        peaks = [ref[t, i, 0:1, :] for i in range(n)]
        peak = functools.reduce(jnp.maximum, peaks)
        total = sum(ref[t, i, 1:2, :] * jnp.exp(peaks[i] - peak) for i in range(n))
        target = sum(ref[t, i, 2:3, :] for i in range(n))
        return peak, total, target

    def put(ref, t, i, values):
        for row, value in enumerate(values):
            ref[t, i, row:row + 1, :] = value

    def stats_y(t):
        for k in range(1, 8):
            g = lax.rem(f + k, 8)
            arrived(stx.at[t, g], sx_r.at[t, g])
        put(sty, t, y, combine(stx, t, 8))
        for k in range(1, Y):
            send(sty.at[t, y], sty.at[t, y], sy_s.at[t, k], sy_r.at[t, k], to_y[k])

    def stats_z(t):
        for k in range(1, Y):
            arrived(sty.at[t, lax.rem(y + Y - k, Y)], sy_r.at[t, k])
        put(stz, t, z, combine(sty, t, Y))
        for k in range(1, Z):
            send(stz.at[t, z], stz.at[t, z], sz_s.at[t, k], sz_r.at[t, k], to_z[k])

    def backward(t):
        for k in range(1, Z):
            arrived(stz.at[t, lax.rem(z + Z - k, Z)], sz_r.at[t, k])
        peak, total, target = combine(stz, t, Z)
        full[t, 0:1, :] = jnp.log(total) + peak - target
        at_label = jnp.exp(target - peak) / total - 1.0
        arrived(e.at[t, fq], e_r.at[t, fq])
        errors_all(t)
        for g in range(8):
            scale = jnp.exp(stx[t, g, 0:1, :] - peak) / total
            value = e[t, g].astype(F32) * scale
            value = jnp.where(rows_of(g) == wanted(t), at_label, value)
            errs[g, :, 256 * t:256 * t + 256] = value.astype(BF16)
        terms = jnp.dot(w[...], errs[:, :, 256 * t:256 * t + 256].reshape(2048, 256),
                        preferred_element_type=F32)
        sb[t] = terms.reshape(4, 96, 256)
        for k in range(1, Y):
            a = lax.rem(y + k, Y)
            send(sb.at[t, a], ry.at[t, k - 1], ry_s.at[t, k - 1], ry_r.at[t, k - 1], to_y[k])

    def reduce_y(t):
        total = sb[t, y]
        for k in range(Y - 1):
            arrived(ry.at[t, k], ry_r.at[t, k])
            total = total + ry[t, k]
        for d in range(2):
            for r in range(4):
                zs[t, 4 * d + r] = total[24 * r:24 * r + 24, 128 * d:128 * d + 128]
        for k in range(1, Z):
            b = lax.rem(z + k, Z)
            send(zs.at[t, b], rz.at[t, k - 1], rz_s.at[t, k - 1], rz_r.at[t, k - 1], to_z[k])

    def home_copy(t):
        return pltpu.make_async_remote_copy(
            src_ref=fs.at[t], dst_ref=fin.at[lax.rem(z, 4)], send_sem=f_s.at[t], recv_sem=f_r.at[lax.rem(z, 4)],
            device_id=home(t), device_id_type=pl.DeviceIdType.MESH)

    def reduce_z(t):
        total = zs[t, z]
        for k in range(Z - 1):
            arrived(rz.at[t, k], rz_r.at[t, k])
            total = total + rz[t, k]
        fs[t] = total
        stays = jnp.logical_and(own_home, x == t)

        @pl.when(stays)
        def _():
            fin[lax.rem(z, 4)] = fs[t]

        @pl.when(jnp.logical_not(stays))
        def _():
            home_copy(t).start()

    forward(0)
    ring_next(2)
    hidden_end(3)
    forward(3)
    errors_2(0)
    stats_y(0)
    hidden_y2(1)
    ring_next(3)
    stats_z(0)
    ring_end()
    forward(2)
    errors_2(3)
    stats_y(3)
    errors_3(0)
    hidden_end(1)
    forward(1)
    backward(0)
    errors_2(2)
    stats_z(3)
    stats_y(2)
    errors_3(3)
    stats_y(1)
    errors_2(1)
    stats_z(2)
    backward(3)
    stats_z(1)
    reduce_y(0)
    errors_3(2)
    errors_3(1)
    backward(2)
    backward(1)
    reduce_y(3)
    reduce_z(0)

    for t in range(X):
        for d in range(2):
            hs[:, 256 * t + 128 * d:256 * t + 128 * d + 128] = h[t, x, pl.ds(4 * c, 4), d].reshape(384, 128)
    for g in range(8):
        grad_out[:, 256 * g:256 * g + 256] = lax.dot_general(
            hs[...], errs[g], (((1,), (1,)), ((), ())), preferred_element_type=F32)
        if g == 1:
            reduce_y(2)
        if g == 3:
            reduce_z(3)
    reduce_y(1)
    reduce_z(2)

    def drain():
        for copy in sends:
            copy.wait_send()
        draining[0] = True
        for core in range(2):
            @pl.when(c == core)
            def _():
                for fn, args in calls[core]:
                    fn(*args)
        draining[0] = False

    drain()
    losses = full[x, 0:1, :]
    loss_out[...] = jnp.where(c == 0, losses[:, 0:128], losses[:, 128:256])
    reduce_z(1)
    for r in range(4):
        @pl.when(jnp.logical_not(jnp.logical_and(own_home, y == r)))
        def _():
            arrived(fin.at[r], f_r.at[r])
    state_out[...] = fin[...].reshape(96, 128).astype(BF16)
    for t in range(X):
        @pl.when(jnp.logical_not(jnp.logical_and(own_home, x == t)))
        def _():
            home_copy(t).wait_send()


def local(hidden_states, head, labels):
    dma = pltpu.SemaphoreType.DMA
    vmem = pltpu.VMEM
    loss, state, grad = pl.pallas_call(
        kernel,
        name="head_loss",
        out_shape=(
            jax.ShapeDtypeStruct((1, 128), F32),
            jax.ShapeDtypeStruct((96, 128), BF16),
            jax.ShapeDtypeStruct((384, 2048), F32),
        ),
        in_specs=[pl.BlockSpec(memory_space=pltpu.HBM)] * 3,
        out_specs=(
            pl.BlockSpec(memory_space=vmem),
            pl.BlockSpec(memory_space=vmem),
            pl.BlockSpec(memory_space=vmem),
        ),
        scratch_shapes=[
            vmem((384, 2048), BF16),
            vmem((8, 384, 256), BF16),
            vmem((2, 2, 2, 192, 256), BF16),
            vmem((256, 3072), BF16),
            vmem((X, Y, Z, 2, 96, 128), BF16),
            vmem((96, 128), BF16),
            vmem((8, 8, 128), jnp.int32),
            vmem((X, 8, 256, 256), BF16),
            vmem((8, 256, 1024), BF16),
            vmem((384, 1024), BF16),
            vmem((X, 8, 8, 256), F32),
            vmem((X, Y, 8, 256), F32),
            vmem((X, Z, 8, 256), F32),
            vmem((X, 8, 256), F32),
            vmem((X, 4, 96, 256), F32),
            vmem((X, Y - 1, 96, 256), F32),
            vmem((X, Z, 24, 128), F32),
            vmem((X, Z - 1, 24, 128), F32),
            vmem((X, 24, 128), F32),
            vmem((4, 24, 128), F32),
            dma((5,)), dma((17,)), dma((8,)), dma((2, 2, 2)), dma((2, 2)),
            dma((X,)), dma((X, 2)), dma((8,)), dma((8,)),
            dma((X, Z)), dma((X, Z)), dma((X, 6)), dma((X, 6)), dma((X, 7)), dma((X, 7)),
            dma((2, 5)), dma((2, 5)), dma((8,)), dma((8,)),
            dma((X, 15)), dma((X, 8)), dma((X, 2, 6)),
            dma((X, 8)), dma((X, 8)), dma((X, Y)), dma((X, Y)), dma((X, Z)), dma((X, Z)),
            dma((X, Y - 1)), dma((X, Y - 1)), dma((X, Z - 1)), dma((X, Z - 1)),
            dma((X,)), dma((4,)), dma((1,)),
        ],
        compiler_params=pltpu.CompilerParams(
            collective_id=0, has_side_effects=True, vmem_limit_bytes=LIMIT * 1024 * 1024),
    )(*(pltpu.with_memory_space_constraint(a, pltpu.HBM)
        for a in (hidden_states.T, head, labels.reshape(1, 128))))
    return (loss.reshape(128), state.T, grad)


def solution(mesh):
    in_specs = (P("fsdp", "vocab"), P("fsdp", "vocab"), P("fsdp"))
    out_specs = (P("fsdp"), P("fsdp", "vocab"), P("fsdp", "vocab"))
    return jax.shard_map(local, mesh=mesh, in_specs=in_specs, out_specs=out_specs, check_vma=False)
```

```python
import functools

import jax
import jax.numpy as jnp
from jax import lax
from jax.experimental import pallas as pl
from jax.experimental.pallas import tpu as pltpu
from jax.sharding import PartitionSpec as P

X, Y, Z = 4, 4, 8
LIMIT = 44
R = 2
HALVES = ((0, 0), (1, 4), (0, 4), (1, 0), (2, 0), (2, 4))
F32, BF16 = jnp.float32, jnp.bfloat16


def kernel(hid, head, labels, loss_out, state_out, grad_out,
           w, wl, relay, wt, h, own, lab, e, errs, hs,
           stx, sty, stz, full, sb, ry, rm, zs, rz, fs, fin,
           load_s, w_s, wl_r, rel_r, w2_r, b1_s, b1_r, lab_s, lab_r,
           hz_s, hz_r, hy_s, hy_r, hd_s, hd_r, hr_s, hr_r, rd_s, rd_r, e_s, e_r, eh_r,
           sx_s, sx_r, sy_s, sy_r, sz_s, sz_r,
           ry_s, ry_r, rz_s, rz_r, f_s, f_r, g_s):
    f, v = lax.axis_index("fsdp"), lax.axis_index("vocab")
    x, c = lax.div(f, 2), lax.rem(f, 2)
    y, z = lax.div(v, Z), lax.rem(v, Z)
    xp, xm, xo = lax.rem(x + 1, X), lax.rem(x + 3, X), lax.rem(x + 2, X)
    yp, ym, yo = lax.rem(y + 1, Y), lax.rem(y + 3, Y), lax.rem(y + 2, Y)
    fp, fm, fo, fq = 2 * xp + c, 2 * xm + c, 2 * xo + c, 2 * x + 1 - c
    ys = [lax.rem(y + k, Y) for k in range(Y)]
    zs_at = [lax.rem(z + k, Z) for k in range(Z)]
    xs = [x, xp, xo, xm]
    group = [[2 * a + d for d in range(2)] for a in xs]
    to_y = [{"fsdp": f, "vocab": Z * a + z} for a in ys]
    to_z = [{"fsdp": f, "vocab": Z * y + b} for b in zs_at]
    sends, calls, draining = [], {0: [], 1: []}, [False]
    role = [None]

    def only(core):
        def wrap(fn):
            def run(*args):
                calls[core].append((fn, args))

                @pl.when(c == core)
                def _():
                    role[0] = core
                    fn(*args)
                    role[0] = None
            run.__name__ = fn.__name__
            return run
        return wrap

    def at_f(g):
        return {"fsdp": g, "vocab": v}

    partner = at_f(fq)

    def send(src, dst, ssem, rsem, device):
        copy = pltpu.make_async_remote_copy(
            src_ref=src, dst_ref=dst, send_sem=ssem, recv_sem=rsem,
            device_id=device, device_id_type=pl.DeviceIdType.MESH)
        if draining[0]:
            copy.wait_send()
            return
        copy.start()
        if role[0] is None:
            sends.append(copy)

    def arrived(dst, rsem):
        if draining[0]:
            return
        pltpu.make_async_remote_copy(
            src_ref=dst, dst_ref=dst, send_sem=g_s.at[0], recv_sem=rsem,
            device_id=partner, device_id_type=pl.DeviceIdType.MESH).wait_recv()

    def home(t):
        return {"fsdp": 2 * t + lax.div(z, 4), "vocab": Z * x + 4 * c + y}

    def origin(r):
        return {"fsdp": 2 * y + lax.div(z, 4), "vocab": Z * lax.rem(z, 4) + 4 * c + r}

    own_home = jnp.logical_and(y == x, z == 4 * c + y)

    load_w = pltpu.make_async_copy(head, w, load_s.at[0])
    load_w.start()
    columns = pl.ds(pl.multiple_of(256 * f, 256), 256)
    load_own = pltpu.make_async_copy(head.at[:, columns], wl.at[f], load_s.at[1])
    load_own.start()

    barrier = pltpu.get_barrier_semaphore()

    def hello(device):
        pl.semaphore_signal(barrier, inc=1, device_id=device, device_id_type=pl.DeviceIdType.MESH)

    for k in range(1, 8):
        hello(at_f(lax.rem(f + k, 8)))
    for k in range(1, Y):
        hello(to_y[k])
    for k in range(1, Z):
        hello(to_z[k])
    for r in range(4):
        @pl.when(jnp.logical_not(jnp.logical_and(own_home, y == r)))
        def _():
            hello(origin(r))

    load_hid = pltpu.make_async_copy(hid, own, load_s.at[2])
    load_hid.start()
    load_lab = pltpu.make_async_copy(labels, lab.at[f, 0:1], load_s.at[3])
    load_lab.start()
    load_mine = pltpu.make_async_copy(hid, h.at[x, y, z, 1], load_s.at[4])

    @pl.when(c == 1)
    def _():
        load_mine.start()

    def begin():
        load_w.wait()
        load_hid.wait()
        load_lab.wait()

        @pl.when(c == 1)
        def _():
            load_mine.wait()

        pl.semaphore_wait(barrier, 7 + 3 + 7 + 4 - own_home.astype(jnp.int32))

    begin()

    for i in range(1, X):
        send(own, h.at[x, y, z, c], b1_s.at[i], b1_r.at[x, c], at_f(group[i][1]))

    def to_carrier():
        send(own, h.at[x, y, z, 0], b1_s.at[0], b1_r.at[x, 0], partner)

    to_carrier = only(0)(to_carrier)
    to_carrier()
    for k in range(1, 8):
        send(lab.at[f], lab.at[f], lab_s.at[k], lab_r.at[f], at_f(lax.rem(f + k, 8)))

    def cols(g):
        return pl.ds(pl.multiple_of(256 * g, 256), 256)

    for d in range(2):
        send(w.at[0:192, cols(2 * xo + d)], relay.at[0, c, d], w_s.at[d], rel_r.at[0, c, d], at_f(group[1][0]))
        send(w.at[192:384, cols(2 * xo + d)], relay.at[1, c, d], w_s.at[2 + d], rel_r.at[1, c, d], at_f(group[3][0]))
    send(w.at[:, cols(fq)], wl.at[f], w_s.at[4], wl_r.at[f], at_f(fq))
    for d in range(2):
        send(w.at[:, cols(2 * xp + d)], wl.at[f], w_s.at[5 + d], wl_r.at[f], at_f(2 * xp + d))
        send(w.at[:, cols(2 * xm + d)], wl.at[f], w_s.at[7 + d], wl_r.at[f], at_f(2 * xm + d))

    def head_in():
        load_own.wait()
        for g in (fq, 2 * xp, 2 * xp + 1, 2 * xm, 2 * xm + 1):
            arrived(wl.at[g], wl_r.at[g])
        for d in range(2):
            arrived(wl.at[2 * xo + d, 0:192], w2_r.at[0, d])
            arrived(wl.at[2 * xo + d, 192:384], w2_r.at[1, d])

    @only(0)
    def relays():
        for d in range(2):
            for o in range(2):
                arrived(relay.at[0, o, d], rel_r.at[0, o, d])
                send(relay.at[0, o, d], wl.at[group[3][o], 0:192],
                     w_s.at[9 + 2 * d + o], w2_r.at[0, o], at_f(group[1][d]))
                arrived(relay.at[1, o, d], rel_r.at[1, o, d])
                send(relay.at[1, o, d], wl.at[group[1][o], 192:384],
                     w_s.at[13 + 2 * d + o], w2_r.at[1, o], at_f(group[3][d]))

    def have(t):
        arrived(h.at[t, y, z, 0], b1_r.at[t, 0])

        @pl.when(x != t)
        def _():
            arrived(h.at[t, y, z, 1], b1_r.at[t, 1])

    @only(1)
    def hidden_z(t):
        have(t)
        block = h.at[t, y, z]
        for k in range(1, Z):
            send(block, block, hz_s.at[t, k], hz_r.at[t, k], to_z[k])

    @only(1)
    def ring_y():
        have(R)
        block = h.at[R, y, z]
        for k in range(1, Y):
            send(block, block, hz_s.at[R, k], hz_r.at[R, k], to_y[k])

    def ring_send(step):
        right, left = zs_at[(1 - step) % Z], zs_at[step - 1]
        low, high = ((0, 4), (0, 4)) if step < 4 else ((0, 2), (2, 4))
        block = h.at[R, low[0]:low[1], right]
        send(block, block, hr_s.at[0, step], hr_r.at[0, step], to_z[1])
        block = h.at[R, high[0]:high[1], left]
        send(block, block, hr_s.at[1, step], hr_r.at[1, step], to_z[7])

    def ring_partner(n, column):
        block = h.at[R, :, column]
        send(block, block, rd_s.at[n], rd_r.at[n], partner)

    @only(1)
    def ring_start():
        for k in range(1, Y):
            arrived(h.at[R, ys[Y - k], z], hz_r.at[R, k])
        ring_send(1)
        ring_partner(0, z)

    @only(1)
    def ring_next(step):
        left, right = zs_at[Z - step], zs_at[step]
        arrived(h.at[R, :, left], hr_r.at[0, step])
        arrived(h.at[R, :, right], hr_r.at[1, step])
        ring_send(step + 1)
        ring_partner(2 * step - 1, left)
        ring_partner(2 * step, right)

    @only(1)
    def ring_end():
        far = zs_at[4]
        arrived(h.at[R, 0:2, far], hr_r.at[0, 4])
        arrived(h.at[R, 2:4, far], hr_r.at[1, 4])
        ring_partner(7, far)

    def to_partner(t, row, low, n):
        block = h.at[t, row, low:low + (4 if n else Z)]
        send(block, block, hd_s.at[t, n], hd_r.at[t, n], partner)

    @only(1)
    def hidden_y(t):
        for k in range(1, Z):
            arrived(h.at[t, y, zs_at[Z - k]], hz_r.at[t, k])
        low, high = h.at[t, y, 0:4], h.at[t, y, 4:8]
        send(low, low, hy_s.at[t, 0], hy_r.at[t, 0], to_y[1])
        send(high, high, hy_s.at[t, 1], hy_r.at[t, 1], to_y[3])
        send(high, high, hy_s.at[t, 4], hy_r.at[t, 4], to_y[1])
        send(low, low, hy_s.at[t, 5], hy_r.at[t, 5], to_y[3])
        to_partner(t, y, 0, 0)

    @only(1)
    def hidden_y2(t):
        block = h.at[t, ym, 0:4]
        arrived(block, hy_r.at[t, 0])
        send(block, block, hy_s.at[t, 2], hy_r.at[t, 2], to_y[1])
        block = h.at[t, yp, 4:8]
        arrived(block, hy_r.at[t, 1])
        send(block, block, hy_s.at[t, 3], hy_r.at[t, 3], to_y[3])
        to_partner(t, ym, 0, 1)
        to_partner(t, yp, 4, 2)

    @only(1)
    def hidden_end(t):
        for n, (row, low) in enumerate(HALVES[2:]):
            row = (ym, yp, yo)[row]
            arrived(h.at[t, row, low:low + 4], hy_r.at[t, (4, 5, 2, 3)[n]])
            to_partner(t, row, low, 3 + n)

    @only(0)
    def hidden_all(t):
        if t == R:
            for n, k in enumerate((0, 7, 1, 6, 2, 5, 3, 4)):
                arrived(h.at[t, :, zs_at[k]], rd_r.at[n])
        else:
            arrived(h.at[t, y], hd_r.at[t, 0])
            for n, (row, low) in enumerate(HALVES):
                arrived(h.at[t, (ym, yp, yo)[row], low:low + 4], hd_r.at[t, 1 + n])

    hidden_z(0)
    hidden_z(3)
    hidden_z(1)
    ring_y()
    ring_start()
    hidden_y(0)
    relays()
    hidden_y2(0)
    hidden_y(3)
    ring_next(1)
    hidden_end(0)
    hidden_y2(3)
    hidden_y(1)
    head_in()
    for g in range(8):
        wt[:, 384 * g:384 * g + 384] = wl[g].T
    for k in range(1, 8):
        g = lax.rem(f + k, 8)
        arrived(lab.at[g], lab_r.at[g])

    def wanted(t):
        return jnp.concatenate([lab[2 * t, 0:1, :], lab[2 * t + 1, 0:1, :]], axis=1)

    def rows_of(g):
        return v * 2048 + g * 256 + lax.broadcasted_iota(jnp.int32, (256, 256), 0)

    def forward(t):
        hidden_all(t)
        states = jnp.concatenate(
            [h[t, :, :, 0].reshape(3072, 128), h[t, :, :, 1].reshape(3072, 128)], axis=1)
        logits = jnp.dot(wt[...], states, preferred_element_type=F32)
        peak = jnp.max(logits, axis=0, keepdims=True)
        shifted = jnp.exp(logits - peak)
        hits = rows_of(f) == wanted(t)
        stx[t, f, 0:1, :] = peak
        stx[t, f, 1:2, :] = jnp.sum(shifted, axis=0, keepdims=True)
        stx[t, f, 2:3, :] = jnp.sum(jnp.where(hits, logits, 0.0), axis=0, keepdims=True)
        e[t, f] = shifted.astype(BF16)
        for k in range(1, 8):
            g = lax.rem(f + k, 8)
            send(stx.at[t, f], stx.at[t, f], sx_s.at[t, k], sx_r.at[t, f], at_f(g))
        low, high, block = e.at[t, f, 0:128], e.at[t, f, 128:256], e.at[t, f]
        send(low, low, e_s.at[t, 0], eh_r.at[t, c, 2], at_f(group[1][0]))
        send(high, high, e_s.at[t, 1], eh_r.at[t, c, 3], at_f(group[3][0]))
        send(high, high, e_s.at[t, 2], eh_r.at[t, c, 4], at_f(group[1][0]))
        send(low, low, e_s.at[t, 3], eh_r.at[t, c, 5], at_f(group[3][0]))
        send(block, block, e_s.at[t, 4], e_r.at[t, f], partner)

    @only(0)
    def errors_2(t):
        for d in range(2):
            block = e.at[t, group[3][d], 0:128]
            arrived(block, eh_r.at[t, d, 2])
            send(block, block, e_s.at[t, 5 + d], eh_r.at[t, d, 0], at_f(group[1][0]))
            block = e.at[t, group[1][d], 128:256]
            arrived(block, eh_r.at[t, d, 3])
            send(block, block, e_s.at[t, 7 + d], eh_r.at[t, d, 1], at_f(group[3][0]))

    @only(0)
    def errors_3(t):
        for d in range(2):
            arrived(e.at[t, group[3][d], 128:256], eh_r.at[t, d, 4])
            arrived(e.at[t, group[1][d], 0:128], eh_r.at[t, d, 5])
            for i, a in enumerate((3, 1)):
                block = e.at[t, group[a][d]]
                send(block, block, e_s.at[t, 9 + 2 * d + i], e_r.at[t, group[a][d]], partner)
        for d in range(2):
            block = e.at[t, group[2][d]]
            arrived(e.at[t, group[2][d], 0:128], eh_r.at[t, d, 0])
            arrived(e.at[t, group[2][d], 128:256], eh_r.at[t, d, 1])
            send(block, block, e_s.at[t, 13 + d], e_r.at[t, group[2][d]], partner)

    @only(1)
    def errors_all(t):
        for a in (3, 1, 2):
            for d in range(2):
                arrived(e.at[t, group[a][d]], e_r.at[t, group[a][d]])

    def combine(ref, t, n):
        peaks = [ref[t, i, 0:1, :] for i in range(n)]
        peak = functools.reduce(jnp.maximum, peaks)
        total = sum(ref[t, i, 1:2, :] * jnp.exp(peaks[i] - peak) for i in range(n))
        target = sum(ref[t, i, 2:3, :] for i in range(n))
        return peak, total, target

    def put(ref, t, i, values):
        for row, value in enumerate(values):
            ref[t, i, row:row + 1, :] = value

    def stats_y(t):
        for k in range(1, 8):
            g = lax.rem(f + k, 8)
            arrived(stx.at[t, g], sx_r.at[t, g])
        put(sty, t, y, combine(stx, t, 8))
        for k in range(1, Y):
            send(sty.at[t, y], sty.at[t, y], sy_s.at[t, k], sy_r.at[t, k], to_y[k])

    def stats_z(t):
        for k in range(1, Y):
            arrived(sty.at[t, lax.rem(y + Y - k, Y)], sy_r.at[t, k])
        put(stz, t, z, combine(sty, t, Y))
        for k in range(1, Z):
            send(stz.at[t, z], stz.at[t, z], sz_s.at[t, k], sz_r.at[t, k], to_z[k])

    def backward(t):
        for k in range(1, Z):
            arrived(stz.at[t, lax.rem(z + Z - k, Z)], sz_r.at[t, k])
        peak, total, target = combine(stz, t, Z)
        full[t, 0:1, :] = jnp.log(total) + peak - target
        at_label = jnp.exp(target - peak) / total - 1.0
        arrived(e.at[t, fq], e_r.at[t, fq])
        errors_all(t)
        for g in range(8):
            scale = jnp.exp(stx[t, g, 0:1, :] - peak) / total
            value = e[t, g].astype(F32) * scale
            value = jnp.where(rows_of(g) == wanted(t), at_label, value)
            errs[g, :, 256 * t:256 * t + 256] = value.astype(BF16)
        terms = jnp.dot(w[...], errs[:, :, 256 * t:256 * t + 256].reshape(2048, 256),
                        preferred_element_type=F32)
        sb[t] = terms.reshape(4, 96, 256)
        send(sb.at[t, yo, 0:48], rm.at[t, 0], ry_s.at[t, 0], ry_r.at[t, 0], to_y[1])
        send(sb.at[t, yo, 48:96], rm.at[t, 1], ry_s.at[t, 1], ry_r.at[t, 1], to_y[3])
        send(sb.at[t, yp, 48:96], ry.at[t, 0, 48:96], ry_s.at[t, 2], ry_r.at[t, 2], to_y[1])
        send(sb.at[t, ym, 0:48], ry.at[t, 1, 0:48], ry_s.at[t, 3], ry_r.at[t, 3], to_y[3])

    def join_y(t):
        arrived(rm.at[t, 0], ry_r.at[t, 0])
        rm[t, 2] = sb[t, yp, 0:48] + rm[t, 0]
        send(rm.at[t, 2], ry.at[t, 0, 0:48], ry_s.at[t, 4], ry_r.at[t, 4], to_y[1])
        arrived(rm.at[t, 1], ry_r.at[t, 1])
        rm[t, 3] = sb[t, ym, 48:96] + rm[t, 1]
        send(rm.at[t, 3], ry.at[t, 1, 48:96], ry_s.at[t, 5], ry_r.at[t, 5], to_y[3])

    def reduce_y(t):
        total = sb[t, y]
        arrived(ry.at[t, 0, 48:96], ry_r.at[t, 2])
        arrived(ry.at[t, 1, 0:48], ry_r.at[t, 3])
        arrived(ry.at[t, 0, 0:48], ry_r.at[t, 4])
        arrived(ry.at[t, 1, 48:96], ry_r.at[t, 5])
        total = total + ry[t, 0] + ry[t, 1]
        for d in range(2):
            for r in range(4):
                zs[t, 4 * d + r] = total[24 * r:24 * r + 24, 128 * d:128 * d + 128]
        for k in range(1, Z):
            b = lax.rem(z + k, Z)
            send(zs.at[t, b], rz.at[t, k - 1], rz_s.at[t, k - 1], rz_r.at[t, k - 1], to_z[k])

    def home_copy(t):
        return pltpu.make_async_remote_copy(
            src_ref=fs.at[t], dst_ref=fin.at[lax.rem(z, 4)], send_sem=f_s.at[t], recv_sem=f_r.at[lax.rem(z, 4)],
            device_id=home(t), device_id_type=pl.DeviceIdType.MESH)

    def reduce_z(t):
        total = zs[t, z]
        for k in range(Z - 1):
            arrived(rz.at[t, k], rz_r.at[t, k])
            total = total + rz[t, k]
        fs[t] = total
        stays = jnp.logical_and(own_home, x == t)

        @pl.when(stays)
        def _():
            fin[lax.rem(z, 4)] = fs[t]

        @pl.when(jnp.logical_not(stays))
        def _():
            home_copy(t).start()

    forward(0)
    ring_next(2)
    hidden_end(3)
    forward(3)
    errors_2(0)
    stats_y(0)
    hidden_y2(1)
    ring_next(3)
    stats_z(0)
    ring_end()
    forward(2)
    errors_2(3)
    stats_y(3)
    errors_3(0)
    hidden_end(1)
    forward(1)
    backward(0)
    errors_2(2)
    stats_z(3)
    stats_y(2)
    join_y(0)
    errors_3(3)
    stats_y(1)
    errors_2(1)
    stats_z(2)
    backward(3)
    stats_z(1)
    reduce_y(0)
    errors_3(2)
    errors_3(1)
    join_y(3)
    backward(2)
    backward(1)
    join_y(2)
    reduce_y(3)

    for t in range(X):
        for d in range(2):
            hs[:, 256 * t + 128 * d:256 * t + 128 * d + 128] = h[t, x, pl.ds(4 * c, 4), d].reshape(384, 128)
    for g in range(8):
        grad_out[:, 256 * g:256 * g + 256] = lax.dot_general(
            hs[...], errs[g], (((1,), (1,)), ((), ())), preferred_element_type=F32)
        if g == 3:
            join_y(1)
            reduce_z(0)
        if g == 5:
            reduce_y(2)
    reduce_z(3)
    reduce_y(1)
    reduce_z(2)

    def drain():
        for copy in sends:
            copy.wait_send()
        draining[0] = True
        for core in range(2):
            @pl.when(c == core)
            def _():
                for fn, args in calls[core]:
                    fn(*args)
        draining[0] = False

    drain()
    losses = full[x, 0:1, :]
    loss_out[...] = jnp.where(c == 0, losses[:, 0:128], losses[:, 128:256])
    reduce_z(1)
    for r in range(4):
        @pl.when(jnp.logical_not(jnp.logical_and(own_home, y == r)))
        def _():
            arrived(fin.at[r], f_r.at[r])
    state_out[...] = fin[...].reshape(96, 128).astype(BF16)
    for t in range(X):
        @pl.when(jnp.logical_not(jnp.logical_and(own_home, x == t)))
        def _():
            home_copy(t).wait_send()


def local(hidden_states, head, labels):
    dma = pltpu.SemaphoreType.DMA
    vmem = pltpu.VMEM
    loss, state, grad = pl.pallas_call(
        kernel,
        name="head_loss",
        out_shape=(
            jax.ShapeDtypeStruct((1, 128), F32),
            jax.ShapeDtypeStruct((96, 128), BF16),
            jax.ShapeDtypeStruct((384, 2048), F32),
        ),
        in_specs=[pl.BlockSpec(memory_space=pltpu.HBM)] * 3,
        out_specs=(
            pl.BlockSpec(memory_space=vmem),
            pl.BlockSpec(memory_space=vmem),
            pl.BlockSpec(memory_space=vmem),
        ),
        scratch_shapes=[
            vmem((384, 2048), BF16),
            vmem((8, 384, 256), BF16),
            vmem((2, 2, 2, 192, 256), BF16),
            vmem((256, 3072), BF16),
            vmem((X, Y, Z, 2, 96, 128), BF16),
            vmem((96, 128), BF16),
            vmem((8, 8, 128), jnp.int32),
            vmem((X, 8, 256, 256), BF16),
            vmem((8, 256, 1024), BF16),
            vmem((384, 1024), BF16),
            vmem((X, 8, 8, 256), F32),
            vmem((X, Y, 8, 256), F32),
            vmem((X, Z, 8, 256), F32),
            vmem((X, 8, 256), F32),
            vmem((X, 4, 96, 256), F32),
            vmem((X, 2, 96, 256), F32),
            vmem((X, 4, 48, 256), F32),
            vmem((X, Z, 24, 128), F32),
            vmem((X, Z - 1, 24, 128), F32),
            vmem((X, 24, 128), F32),
            vmem((4, 24, 128), F32),
            dma((5,)), dma((17,)), dma((8,)), dma((2, 2, 2)), dma((2, 2)),
            dma((X,)), dma((X, 2)), dma((8,)), dma((8,)),
            dma((X, Z)), dma((X, Z)), dma((X, 6)), dma((X, 6)), dma((X, 7)), dma((X, 7)),
            dma((2, 5)), dma((2, 5)), dma((8,)), dma((8,)),
            dma((X, 15)), dma((X, 8)), dma((X, 2, 6)),
            dma((X, 8)), dma((X, 8)), dma((X, Y)), dma((X, Y)), dma((X, Z)), dma((X, Z)),
            dma((X, 6)), dma((X, 6)), dma((X, Z - 1)), dma((X, Z - 1)),
            dma((X,)), dma((4,)), dma((1,)),
        ],
        compiler_params=pltpu.CompilerParams(
            collective_id=0, has_side_effects=True, vmem_limit_bytes=LIMIT * 1024 * 1024),
    )(*(pltpu.with_memory_space_constraint(a, pltpu.HBM)
        for a in (hidden_states.T, head, labels.reshape(1, 128))))
    return (loss.reshape(128), state.T, grad)


def solution(mesh):
    in_specs = (P("fsdp", "vocab"), P("fsdp", "vocab"), P("fsdp"))
    out_specs = (P("fsdp"), P("fsdp", "vocab"), P("fsdp", "vocab"))
    return jax.shard_map(local, mesh=mesh, in_specs=in_specs, out_specs=out_specs, check_vma=False)
```

```python
import functools

import jax
import jax.numpy as jnp
from jax import lax
from jax.experimental import pallas as pl
from jax.experimental.pallas import tpu as pltpu
from jax.sharding import PartitionSpec as P

X, Y, Z = 4, 4, 8
LIMIT = 44
R = 2
FAR_Z, FAR_Y = (4, 3, 5, 2, 6, 1, 7), (2, 1, 3)
HALVES = ((0, 0), (1, 4), (0, 4), (1, 0), (2, 0), (2, 4))
F32, BF16 = jnp.float32, jnp.bfloat16


def kernel(hid, head, labels, loss_out, state_out, grad_out,
           w, wl, relay, wt, h, own, lab, e, errs, hs,
           stx, sty, stz, full, sb, ry, rm, zs, rz, fs, fin,
           load_s, w_s, wl_r, rel_r, w2_r, b1_s, b1_r, lab_s, lab_r,
           hz_s, hz_r, hy_s, hy_r, hd_s, hd_r, hr_s, hr_r, rd_s, rd_r, e_s, e_r, eh_r,
           sx_s, sx_r, sy_s, sy_r, sz_s, sz_r,
           ry_s, ry_r, rz_s, rz_r, f_s, f_r, g_s):
    f, v = lax.axis_index("fsdp"), lax.axis_index("vocab")
    x, c = lax.div(f, 2), lax.rem(f, 2)
    y, z = lax.div(v, Z), lax.rem(v, Z)
    xp, xm, xo = lax.rem(x + 1, X), lax.rem(x + 3, X), lax.rem(x + 2, X)
    yp, ym, yo = lax.rem(y + 1, Y), lax.rem(y + 3, Y), lax.rem(y + 2, Y)
    fp, fm, fo, fq = 2 * xp + c, 2 * xm + c, 2 * xo + c, 2 * x + 1 - c
    ys = [lax.rem(y + k, Y) for k in range(Y)]
    zs_at = [lax.rem(z + k, Z) for k in range(Z)]
    xs = [x, xp, xo, xm]
    group = [[2 * a + d for d in range(2)] for a in xs]
    to_y = [{"fsdp": f, "vocab": Z * a + z} for a in ys]
    to_z = [{"fsdp": f, "vocab": Z * y + b} for b in zs_at]
    sends, calls, draining = [], {0: [], 1: []}, [False]
    role = [None]

    def only(core):
        def wrap(fn):
            def run(*args):
                calls[core].append((fn, args))

                @pl.when(c == core)
                def _():
                    role[0] = core
                    fn(*args)
                    role[0] = None
            run.__name__ = fn.__name__
            return run
        return wrap

    def at_f(g):
        return {"fsdp": g, "vocab": v}

    partner = at_f(fq)

    def send(src, dst, ssem, rsem, device):
        copy = pltpu.make_async_remote_copy(
            src_ref=src, dst_ref=dst, send_sem=ssem, recv_sem=rsem,
            device_id=device, device_id_type=pl.DeviceIdType.MESH)
        if draining[0]:
            copy.wait_send()
            return
        copy.start()
        if role[0] is None:
            sends.append(copy)

    def arrived(dst, rsem):
        if draining[0]:
            return
        pltpu.make_async_remote_copy(
            src_ref=dst, dst_ref=dst, send_sem=g_s.at[0], recv_sem=rsem,
            device_id=partner, device_id_type=pl.DeviceIdType.MESH).wait_recv()

    def home(t):
        return {"fsdp": 2 * t + lax.div(z, 4), "vocab": Z * x + 4 * c + y}

    def origin(r):
        return {"fsdp": 2 * y + lax.div(z, 4), "vocab": Z * lax.rem(z, 4) + 4 * c + r}

    own_home = jnp.logical_and(y == x, z == 4 * c + y)

    load_w = pltpu.make_async_copy(head, w, load_s.at[0])
    load_w.start()
    columns = pl.ds(pl.multiple_of(256 * f, 256), 256)
    load_own = pltpu.make_async_copy(head.at[:, columns], wl.at[f], load_s.at[1])
    load_own.start()

    barrier = pltpu.get_barrier_semaphore()

    def hello(device):
        pl.semaphore_signal(barrier, inc=1, device_id=device, device_id_type=pl.DeviceIdType.MESH)

    for k in range(1, 8):
        hello(at_f(lax.rem(f + k, 8)))
    for k in FAR_Y:
        hello(to_y[k])
    for k in FAR_Z:
        hello(to_z[k])
    for r in range(4):
        @pl.when(jnp.logical_not(jnp.logical_and(own_home, y == r)))
        def _():
            hello(origin(r))

    load_hid = pltpu.make_async_copy(hid, own, load_s.at[2])
    load_hid.start()
    load_lab = pltpu.make_async_copy(labels, lab.at[f, 0:1], load_s.at[3])
    load_lab.start()
    load_mine = pltpu.make_async_copy(hid, h.at[x, y, z, 1], load_s.at[4])

    @pl.when(c == 1)
    def _():
        load_mine.start()

    def begin():
        load_w.wait()
        load_hid.wait()
        load_lab.wait()

        @pl.when(c == 1)
        def _():
            load_mine.wait()

        pl.semaphore_wait(barrier, 7 + 3 + 7 + 4 - own_home.astype(jnp.int32))

    begin()

    for i in range(1, X):
        send(own, h.at[x, y, z, c], b1_s.at[i], b1_r.at[x, c], at_f(group[i][1]))

    def to_carrier():
        send(own, h.at[x, y, z, 0], b1_s.at[0], b1_r.at[x, 0], partner)

    to_carrier = only(0)(to_carrier)
    to_carrier()
    for k in range(1, 8):
        send(lab.at[f], lab.at[f], lab_s.at[k], lab_r.at[f], at_f(lax.rem(f + k, 8)))

    def cols(g):
        return pl.ds(pl.multiple_of(256 * g, 256), 256)

    for d in range(2):
        send(w.at[0:192, cols(2 * xo + d)], relay.at[0, c, d], w_s.at[d], rel_r.at[0, c, d], at_f(group[1][0]))
        send(w.at[192:384, cols(2 * xo + d)], relay.at[1, c, d], w_s.at[2 + d], rel_r.at[1, c, d], at_f(group[3][0]))
    send(w.at[:, cols(fq)], wl.at[f], w_s.at[4], wl_r.at[f], at_f(fq))
    for d in range(2):
        send(w.at[:, cols(2 * xp + d)], wl.at[f], w_s.at[5 + d], wl_r.at[f], at_f(2 * xp + d))
        send(w.at[:, cols(2 * xm + d)], wl.at[f], w_s.at[7 + d], wl_r.at[f], at_f(2 * xm + d))

    def head_in():
        load_own.wait()
        for g in (fq, 2 * xp, 2 * xp + 1, 2 * xm, 2 * xm + 1):
            arrived(wl.at[g], wl_r.at[g])
        for d in range(2):
            arrived(wl.at[2 * xo + d, 0:192], w2_r.at[0, d])
            arrived(wl.at[2 * xo + d, 192:384], w2_r.at[1, d])

    @only(0)
    def relays():
        for d in range(2):
            for o in range(2):
                arrived(relay.at[0, o, d], rel_r.at[0, o, d])
                send(relay.at[0, o, d], wl.at[group[3][o], 0:192],
                     w_s.at[9 + 2 * d + o], w2_r.at[0, o], at_f(group[1][d]))
                arrived(relay.at[1, o, d], rel_r.at[1, o, d])
                send(relay.at[1, o, d], wl.at[group[1][o], 192:384],
                     w_s.at[13 + 2 * d + o], w2_r.at[1, o], at_f(group[3][d]))

    def have(t):
        arrived(h.at[t, y, z, 0], b1_r.at[t, 0])

        @pl.when(x != t)
        def _():
            arrived(h.at[t, y, z, 1], b1_r.at[t, 1])

    @only(1)
    def hidden_z(t):
        have(t)
        block = h.at[t, y, z]
        for k in FAR_Z:
            send(block, block, hz_s.at[t, k], hz_r.at[t, k], to_z[k])

    @only(1)
    def ring_y():
        have(R)
        block = h.at[R, y, z]
        for k in FAR_Y:
            send(block, block, hz_s.at[R, k], hz_r.at[R, k], to_y[k])

    def ring_send(step):
        right, left = zs_at[(1 - step) % Z], zs_at[step - 1]
        low, high = ((0, 4), (0, 4)) if step < 4 else ((0, 2), (2, 4))
        block = h.at[R, low[0]:low[1], right]
        send(block, block, hr_s.at[0, step], hr_r.at[0, step], to_z[1])
        block = h.at[R, high[0]:high[1], left]
        send(block, block, hr_s.at[1, step], hr_r.at[1, step], to_z[7])

    def ring_partner(n, column):
        block = h.at[R, :, column]
        send(block, block, rd_s.at[n], rd_r.at[n], partner)

    @only(1)
    def ring_start():
        for k in range(1, Y):
            arrived(h.at[R, ys[Y - k], z], hz_r.at[R, k])
        ring_send(1)
        ring_partner(0, z)

    @only(1)
    def ring_next(step):
        left, right = zs_at[Z - step], zs_at[step]
        arrived(h.at[R, :, left], hr_r.at[0, step])
        arrived(h.at[R, :, right], hr_r.at[1, step])
        ring_send(step + 1)
        ring_partner(2 * step - 1, left)
        ring_partner(2 * step, right)

    @only(1)
    def ring_end():
        far = zs_at[4]
        arrived(h.at[R, 0:2, far], hr_r.at[0, 4])
        arrived(h.at[R, 2:4, far], hr_r.at[1, 4])
        ring_partner(7, far)

    def to_partner(t, row, low, n):
        block = h.at[t, row, low:low + (4 if n else Z)]
        send(block, block, hd_s.at[t, n], hd_r.at[t, n], partner)

    @only(1)
    def hidden_y(t):
        for k in range(1, Z):
            arrived(h.at[t, y, zs_at[Z - k]], hz_r.at[t, k])
        low, high = h.at[t, y, 0:4], h.at[t, y, 4:8]
        send(low, low, hy_s.at[t, 0], hy_r.at[t, 0], to_y[1])
        send(high, high, hy_s.at[t, 1], hy_r.at[t, 1], to_y[3])
        send(high, high, hy_s.at[t, 4], hy_r.at[t, 4], to_y[1])
        send(low, low, hy_s.at[t, 5], hy_r.at[t, 5], to_y[3])
        to_partner(t, y, 0, 0)

    @only(1)
    def hidden_y2(t):
        block = h.at[t, ym, 0:4]
        arrived(block, hy_r.at[t, 0])
        send(block, block, hy_s.at[t, 2], hy_r.at[t, 2], to_y[1])
        block = h.at[t, yp, 4:8]
        arrived(block, hy_r.at[t, 1])
        send(block, block, hy_s.at[t, 3], hy_r.at[t, 3], to_y[3])
        to_partner(t, ym, 0, 1)
        to_partner(t, yp, 4, 2)

    @only(1)
    def hidden_end(t):
        for n, (row, low) in enumerate(HALVES[2:]):
            row = (ym, yp, yo)[row]
            arrived(h.at[t, row, low:low + 4], hy_r.at[t, (4, 5, 2, 3)[n]])
            to_partner(t, row, low, 3 + n)

    @only(0)
    def hidden_all(t):
        if t == R:
            for n, k in enumerate((0, 7, 1, 6, 2, 5, 3, 4)):
                arrived(h.at[t, :, zs_at[k]], rd_r.at[n])
        else:
            arrived(h.at[t, y], hd_r.at[t, 0])
            for n, (row, low) in enumerate(HALVES):
                arrived(h.at[t, (ym, yp, yo)[row], low:low + 4], hd_r.at[t, 1 + n])

    hidden_z(0)
    hidden_z(3)
    hidden_z(1)
    ring_y()
    ring_start()
    hidden_y(0)
    relays()
    hidden_y2(0)
    hidden_y(3)
    ring_next(1)
    hidden_end(0)
    hidden_y2(3)
    hidden_y(1)
    head_in()
    for g in range(8):
        wt[:, 384 * g:384 * g + 384] = wl[g].T
    for k in range(1, 8):
        g = lax.rem(f + k, 8)
        arrived(lab.at[g], lab_r.at[g])

    def wanted(t):
        return jnp.concatenate([lab[2 * t, 0:1, :], lab[2 * t + 1, 0:1, :]], axis=1)

    def rows_of(g):
        return v * 2048 + g * 256 + lax.broadcasted_iota(jnp.int32, (256, 256), 0)

    def forward(t):
        hidden_all(t)
        states = jnp.concatenate(
            [h[t, :, :, 0].reshape(3072, 128), h[t, :, :, 1].reshape(3072, 128)], axis=1)
        logits = jnp.dot(wt[...], states, preferred_element_type=F32)
        peak = jnp.max(logits, axis=0, keepdims=True)
        shifted = jnp.exp(logits - peak)
        hits = rows_of(f) == wanted(t)
        stx[t, f, 0:1, :] = peak
        stx[t, f, 1:2, :] = jnp.sum(shifted, axis=0, keepdims=True)
        stx[t, f, 2:3, :] = jnp.sum(jnp.where(hits, logits, 0.0), axis=0, keepdims=True)
        e[t, f] = shifted.astype(BF16)
        for k in range(1, 8):
            g = lax.rem(f + k, 8)
            send(stx.at[t, f], stx.at[t, f], sx_s.at[t, k], sx_r.at[t, f], at_f(g))
        low, high, block = e.at[t, f, 0:128], e.at[t, f, 128:256], e.at[t, f]
        send(low, low, e_s.at[t, 0], eh_r.at[t, c, 2], at_f(group[1][0]))
        send(high, high, e_s.at[t, 1], eh_r.at[t, c, 3], at_f(group[3][0]))
        send(high, high, e_s.at[t, 2], eh_r.at[t, c, 4], at_f(group[1][0]))
        send(low, low, e_s.at[t, 3], eh_r.at[t, c, 5], at_f(group[3][0]))
        send(block, block, e_s.at[t, 4], e_r.at[t, f], partner)

    @only(0)
    def errors_2(t):
        for d in range(2):
            block = e.at[t, group[3][d], 0:128]
            arrived(block, eh_r.at[t, d, 2])
            send(block, block, e_s.at[t, 5 + d], eh_r.at[t, d, 0], at_f(group[1][0]))
            block = e.at[t, group[1][d], 128:256]
            arrived(block, eh_r.at[t, d, 3])
            send(block, block, e_s.at[t, 7 + d], eh_r.at[t, d, 1], at_f(group[3][0]))

    @only(0)
    def errors_3(t):
        for d in range(2):
            arrived(e.at[t, group[3][d], 128:256], eh_r.at[t, d, 4])
            arrived(e.at[t, group[1][d], 0:128], eh_r.at[t, d, 5])
            for i, a in enumerate((3, 1)):
                block = e.at[t, group[a][d]]
                send(block, block, e_s.at[t, 9 + 2 * d + i], e_r.at[t, group[a][d]], partner)
        for d in range(2):
            block = e.at[t, group[2][d]]
            arrived(e.at[t, group[2][d], 0:128], eh_r.at[t, d, 0])
            arrived(e.at[t, group[2][d], 128:256], eh_r.at[t, d, 1])
            send(block, block, e_s.at[t, 13 + d], e_r.at[t, group[2][d]], partner)

    @only(1)
    def errors_all(t):
        for a in (3, 1, 2):
            for d in range(2):
                arrived(e.at[t, group[a][d]], e_r.at[t, group[a][d]])

    def combine(ref, t, n):
        peaks = [ref[t, i, 0:1, :] for i in range(n)]
        peak = functools.reduce(jnp.maximum, peaks)
        total = sum(ref[t, i, 1:2, :] * jnp.exp(peaks[i] - peak) for i in range(n))
        target = sum(ref[t, i, 2:3, :] for i in range(n))
        return peak, total, target

    def put(ref, t, i, values):
        for row, value in enumerate(values):
            ref[t, i, row:row + 1, :] = value

    def stats_y(t):
        for k in range(1, 8):
            g = lax.rem(f + k, 8)
            arrived(stx.at[t, g], sx_r.at[t, g])
        put(sty, t, y, combine(stx, t, 8))
        for k in FAR_Y:
            send(sty.at[t, y], sty.at[t, y], sy_s.at[t, k], sy_r.at[t, k], to_y[k])

    def stats_z(t):
        for k in range(1, Y):
            arrived(sty.at[t, lax.rem(y + Y - k, Y)], sy_r.at[t, k])
        put(stz, t, z, combine(sty, t, Y))
        for k in FAR_Z:
            send(stz.at[t, z], stz.at[t, z], sz_s.at[t, k], sz_r.at[t, k], to_z[k])

    def backward(t):
        for k in range(1, Z):
            arrived(stz.at[t, lax.rem(z + Z - k, Z)], sz_r.at[t, k])
        peak, total, target = combine(stz, t, Z)
        full[t, 0:1, :] = jnp.log(total) + peak - target
        at_label = jnp.exp(target - peak) / total - 1.0
        arrived(e.at[t, fq], e_r.at[t, fq])
        errors_all(t)
        for g in range(8):
            scale = jnp.exp(stx[t, g, 0:1, :] - peak) / total
            value = e[t, g].astype(F32) * scale
            value = jnp.where(rows_of(g) == wanted(t), at_label, value)
            errs[g, :, 256 * t:256 * t + 256] = value.astype(BF16)
        terms = jnp.dot(w[...], errs[:, :, 256 * t:256 * t + 256].reshape(2048, 256),
                        preferred_element_type=F32)
        sb[t] = terms.reshape(4, 96, 256)
        send(sb.at[t, yo, 0:48], rm.at[t, 0], ry_s.at[t, 0], ry_r.at[t, 0], to_y[1])
        send(sb.at[t, yo, 48:96], rm.at[t, 1], ry_s.at[t, 1], ry_r.at[t, 1], to_y[3])
        send(sb.at[t, yp, 48:96], ry.at[t, 0, 48:96], ry_s.at[t, 2], ry_r.at[t, 2], to_y[1])
        send(sb.at[t, ym, 0:48], ry.at[t, 1, 0:48], ry_s.at[t, 3], ry_r.at[t, 3], to_y[3])

    def join_y(t):
        arrived(rm.at[t, 0], ry_r.at[t, 0])
        rm[t, 2] = sb[t, yp, 0:48] + rm[t, 0]
        send(rm.at[t, 2], ry.at[t, 0, 0:48], ry_s.at[t, 4], ry_r.at[t, 4], to_y[1])
        arrived(rm.at[t, 1], ry_r.at[t, 1])
        rm[t, 3] = sb[t, ym, 48:96] + rm[t, 1]
        send(rm.at[t, 3], ry.at[t, 1, 48:96], ry_s.at[t, 5], ry_r.at[t, 5], to_y[3])

    def reduce_y(t):
        total = sb[t, y]
        arrived(ry.at[t, 0, 48:96], ry_r.at[t, 2])
        arrived(ry.at[t, 1, 0:48], ry_r.at[t, 3])
        arrived(ry.at[t, 0, 0:48], ry_r.at[t, 4])
        arrived(ry.at[t, 1, 48:96], ry_r.at[t, 5])
        total = total + ry[t, 0] + ry[t, 1]
        for d in range(2):
            for r in range(4):
                zs[t, 4 * d + r] = total[24 * r:24 * r + 24, 128 * d:128 * d + 128]
        for k in FAR_Z:
            b = lax.rem(z + k, Z)
            send(zs.at[t, b], rz.at[t, k - 1], rz_s.at[t, k - 1], rz_r.at[t, k - 1], to_z[k])

    def home_copy(t):
        return pltpu.make_async_remote_copy(
            src_ref=fs.at[t], dst_ref=fin.at[lax.rem(z, 4)], send_sem=f_s.at[t], recv_sem=f_r.at[lax.rem(z, 4)],
            device_id=home(t), device_id_type=pl.DeviceIdType.MESH)

    def reduce_z(t):
        total = zs[t, z]
        for k in range(Z - 1):
            arrived(rz.at[t, k], rz_r.at[t, k])
            total = total + rz[t, k]
        fs[t] = total
        stays = jnp.logical_and(own_home, x == t)

        @pl.when(stays)
        def _():
            fin[lax.rem(z, 4)] = fs[t]

        @pl.when(jnp.logical_not(stays))
        def _():
            home_copy(t).start()

    forward(0)
    ring_next(2)
    hidden_end(3)
    forward(3)
    errors_2(0)
    stats_y(0)
    hidden_y2(1)
    ring_next(3)
    stats_z(0)
    ring_end()
    forward(2)
    errors_2(3)
    stats_y(3)
    errors_3(0)
    hidden_end(1)
    forward(1)
    backward(0)
    errors_2(2)
    stats_z(3)
    stats_y(2)
    join_y(0)
    errors_3(3)
    stats_y(1)
    errors_2(1)
    stats_z(2)
    backward(3)
    stats_z(1)
    reduce_y(0)
    errors_3(2)
    errors_3(1)
    join_y(3)
    backward(2)
    backward(1)
    join_y(2)
    reduce_y(3)

    for t in range(X):
        for d in range(2):
            hs[:, 256 * t + 128 * d:256 * t + 128 * d + 128] = h[t, x, pl.ds(4 * c, 4), d].reshape(384, 128)
    for g in range(8):
        grad_out[:, 256 * g:256 * g + 256] = lax.dot_general(
            hs[...], errs[g], (((1,), (1,)), ((), ())), preferred_element_type=F32)
        if g == 3:
            join_y(1)
            reduce_z(0)
        if g == 5:
            reduce_y(2)
    reduce_z(3)
    reduce_y(1)
    reduce_z(2)

    def drain():
        for copy in sends:
            copy.wait_send()
        draining[0] = True
        for core in range(2):
            @pl.when(c == core)
            def _():
                for fn, args in calls[core]:
                    fn(*args)
        draining[0] = False

    drain()
    losses = full[x, 0:1, :]
    loss_out[...] = jnp.where(c == 0, losses[:, 0:128], losses[:, 128:256])
    reduce_z(1)
    for r in range(4):
        @pl.when(jnp.logical_not(jnp.logical_and(own_home, y == r)))
        def _():
            arrived(fin.at[r], f_r.at[r])
    state_out[...] = fin[...].reshape(96, 128).astype(BF16)
    for t in range(X):
        @pl.when(jnp.logical_not(jnp.logical_and(own_home, x == t)))
        def _():
            home_copy(t).wait_send()


def local(hidden_states, head, labels):
    dma = pltpu.SemaphoreType.DMA
    vmem = pltpu.VMEM
    loss, state, grad = pl.pallas_call(
        kernel,
        name="head_loss",
        out_shape=(
            jax.ShapeDtypeStruct((1, 128), F32),
            jax.ShapeDtypeStruct((96, 128), BF16),
            jax.ShapeDtypeStruct((384, 2048), F32),
        ),
        in_specs=[pl.BlockSpec(memory_space=pltpu.HBM)] * 3,
        out_specs=(
            pl.BlockSpec(memory_space=vmem),
            pl.BlockSpec(memory_space=vmem),
            pl.BlockSpec(memory_space=vmem),
        ),
        scratch_shapes=[
            vmem((384, 2048), BF16),
            vmem((8, 384, 256), BF16),
            vmem((2, 2, 2, 192, 256), BF16),
            vmem((256, 3072), BF16),
            vmem((X, Y, Z, 2, 96, 128), BF16),
            vmem((96, 128), BF16),
            vmem((8, 8, 128), jnp.int32),
            vmem((X, 8, 256, 256), BF16),
            vmem((8, 256, 1024), BF16),
            vmem((384, 1024), BF16),
            vmem((X, 8, 8, 256), F32),
            vmem((X, Y, 8, 256), F32),
            vmem((X, Z, 8, 256), F32),
            vmem((X, 8, 256), F32),
            vmem((X, 4, 96, 256), F32),
            vmem((X, 2, 96, 256), F32),
            vmem((X, 4, 48, 256), F32),
            vmem((X, Z, 24, 128), F32),
            vmem((X, Z - 1, 24, 128), F32),
            vmem((X, 24, 128), F32),
            vmem((4, 24, 128), F32),
            dma((5,)), dma((17,)), dma((8,)), dma((2, 2, 2)), dma((2, 2)),
            dma((X,)), dma((X, 2)), dma((8,)), dma((8,)),
            dma((X, Z)), dma((X, Z)), dma((X, 6)), dma((X, 6)), dma((X, 7)), dma((X, 7)),
            dma((2, 5)), dma((2, 5)), dma((8,)), dma((8,)),
            dma((X, 15)), dma((X, 8)), dma((X, 2, 6)),
            dma((X, 8)), dma((X, 8)), dma((X, Y)), dma((X, Y)), dma((X, Z)), dma((X, Z)),
            dma((X, 6)), dma((X, 6)), dma((X, Z - 1)), dma((X, Z - 1)),
            dma((X,)), dma((4,)), dma((1,)),
        ],
        compiler_params=pltpu.CompilerParams(
            collective_id=0, has_side_effects=True, vmem_limit_bytes=LIMIT * 1024 * 1024),
    )(*(pltpu.with_memory_space_constraint(a, pltpu.HBM)
        for a in (hidden_states.T, head, labels.reshape(1, 128))))
    return (loss.reshape(128), state.T, grad)


def solution(mesh):
    in_specs = (P("fsdp", "vocab"), P("fsdp", "vocab"), P("fsdp"))
    out_specs = (P("fsdp"), P("fsdp", "vocab"), P("fsdp", "vocab"))
    return jax.shard_map(local, mesh=mesh, in_specs=in_specs, out_specs=out_specs, check_vma=False)
```
